256 devices in a mesh: task: 128 (over x, y, z), shard: 2 (over core).
Axes of the slice: x: 4, y: 4, z: 8, core: 2. Of those that a mesh axis runs over, the one named last changes fastest.
Arguments:
- tokens: bfloat16 [128, 512, 1024], P('task'), may hold values from -6 to 6
- targets: bfloat16 [128, 512, 1024], P('task'), may hold values from -6 to 6
- meta_tokens: bfloat16 [128, 512, 1024], P('task'), may hold values from -6 to 6
- meta_targets: bfloat16 [128, 512, 1024], P('task'), may hold values from -6 to 6
- gate_weight: bfloat16 [128, 1024, 1536], P('task', None, 'shard'), may hold values from -0.1875 to 0.1875
- up_weight: bfloat16 [128, 1024, 1536], P('task', None, 'shard'), may hold values from -0.1875 to 0.1875
- down_weight: bfloat16 [128, 1536, 1024], P('task', 'shard'), may hold values from -0.15625 to 0.15625
- task_step: int32 [128], P('task'), may hold values from 0 to 9999
- hidden_state: float32 [128, 3, 512], P('task'), may hold values from -3 to 3
- cell_state: float32 [128, 3, 512], P('task'), may hold values from -6 to 6
- recurrent_weight: float32 [512, 2048], P('task'), may hold values from -0.25 to 0.25
- input_weight: float32 [3, 2048], replicated, may hold values from -3.5 to 3.5
- lstm_bias: float32 [2048], replicated, may hold values from -3 to 3
- context_weight: float32 [512, 5], replicated, may hold values from -0.25 to 0.25
- mlp_weight: float32 [3, 4], replicated, may hold values from -4 to 4
Outputs:
- gate_update: bfloat16 [128, 1024, 1536], P('task', None, 'shard')
- up_update: bfloat16 [128, 1024, 1536], P('task', None, 'shard')
- down_update: bfloat16 [128, 1536, 1024], P('task', 'shard')
- new_hidden: float32 [128, 3, 512], P('task')
- new_cell: float32 [128, 3, 512], P('task')
- meta_loss: float32 [], replicated
The draws below stay inside these ranges and needn't reach their ends.
All inputs are finite; a program needn't handle non-finite values.
Results may differ from the reference program's by a relative error of at most 0.0056.
Values sent between devices are 32-bit elements; how exact they have to be, the bound alone decides.
No kernel may reach another device: no remote copies, remote signals or barrier semaphores. Data moves between devices by JAX's collectives and lax.ppermute only.
A program may use at most 128 MiB of HBM per device.

```python
import jax
import jax.numpy as jnp
from jax import lax

D = 1024
FF = 1536
H = 512
MLP_H = 4
FEAT = 3
STEPS = 10000
TOK = 512
TASKS = 128


def touch_ends(array, own_key, smallest, top_value):
    dims = array.shape
    spot = [jax.random.randint(jax.random.fold_in(own_key, axis), (), 0, dims[axis]) for axis in range(len(dims))]
    array = array.at[tuple(spot)].set(smallest)
    longest = dims.index(max(dims))
    spot[longest] = (spot[longest] + 1) % dims[longest]
    return array.at[tuple(spot)].set(top_value)


def block_scale(rng, extent, shards, low, top_value):
    factor_of, own = 1.0, jax.random.fold_in(rng, 6)
    for dim, shards_of in shards:
        steps = jnp.exp(jax.random.uniform(jax.random.fold_in(own, dim), (shards_of,), jnp.float32, low / len(shards), top_value / len(shards)))
        factor_of = factor_of * jnp.repeat(steps, extent[dim] // shards_of).reshape([-1 if axis == dim else 1 for axis in range(len(extent))])
    return factor_of


def gaussian(own_key, dims, scale, reach, split=(), kind=jnp.bfloat16):
    drawn = jax.random.normal(own_key, dims, jnp.float32) * scale
    if len(split) > 0:
        drawn = block_scale(own_key, dims, split, -0.22, 0.18) * drawn
    return jnp.clip(drawn, min=-reach, max=reach).astype(kind)


def setup_inputs(seed: int = 0) -> dict:
    key_of = jax.random.split(jax.random.key(seed), 16)
    tokens = gaussian(key_of[0], (TASKS, TOK, D), 1.0, 6.0, ((0, 128),))
    targets = gaussian(key_of[1], (TASKS, TOK, D), 1.0, 6.0, ((0, 128),))
    meta_tokens = gaussian(key_of[2], (TASKS, TOK, D), 1.0, 6.0, ((0, 128),))
    meta_targets = gaussian(key_of[3], (TASKS, TOK, D), 1.0, 6.0, ((0, 128),))
    gate_weight = gaussian(key_of[4], (TASKS, D, FF), D ** -0.5, 0.1875, ((0, 128), (2, 2)))
    up_weight = gaussian(key_of[5], (TASKS, D, FF), D ** -0.5, 0.1875, ((0, 128), (2, 2)))
    down_weight = gaussian(key_of[6], (TASKS, FF, D), FF ** -0.5, 0.15625, ((0, 128), (1, 2)))
    task_step = touch_ends(jax.random.randint(key_of[7], (TASKS,), 0, STEPS), jax.random.fold_in(key_of[7], 1), 0, STEPS - 1).astype(jnp.int32)
    hidden_state = gaussian(key_of[8], (TASKS, 3, H), 0.5, 3.0, ((0, 128),), jnp.float32)
    cell_state = gaussian(key_of[9], (TASKS, 3, H), 1.0, 6.0, ((0, 128),), jnp.float32)
    recurrent_weight = gaussian(key_of[10], (H, 4 * H), H ** -0.5, 0.25, ((0, 128),), jnp.float32)
    input_weight = gaussian(key_of[11], (FEAT, 4 * H), FEAT ** -0.5, 3.5, (), jnp.float32)
    lstm_bias = gaussian(key_of[12], (4 * H,), 0.5, 3.0, (), jnp.float32)
    context_weight = gaussian(key_of[13], (H, MLP_H + 1), H ** -0.5, 0.25, (), jnp.float32)
    mlp_weight = gaussian(key_of[14], (3, MLP_H), 1.0, 4.0, (), jnp.float32)
    return dict(tokens=tokens, targets=targets, meta_tokens=meta_tokens, meta_targets=meta_targets, gate_weight=gate_weight, up_weight=up_weight, down_weight=down_weight, task_step=task_step, hidden_state=hidden_state, cell_state=cell_state, recurrent_weight=recurrent_weight, input_weight=input_weight, lstm_bias=lstm_bias, context_weight=context_weight, mlp_weight=mlp_weight)


highest = lax.Precision.HIGHEST
epsilon = 1e-06
rate_factor = 0.1

def block_forward(inputs, w_gate, w_up, w_down):
    gate_pre = jnp.dot(inputs, w_gate, preferred_element_type=jnp.float32)
    up_pre = jnp.dot(inputs, w_up, preferred_element_type=jnp.float32)
    sigmoid_gate = jax.nn.sigmoid(gate_pre)
    activated = (gate_pre * sigmoid_gate * up_pre).astype(jnp.bfloat16)
    output = jnp.dot(activated, w_down, preferred_element_type=jnp.float32)
    return (gate_pre, up_pre, sigmoid_gate, activated, output)

def block_grads(inputs, w_down, gate_pre, up_pre, sigmoid_gate, activated, d_out):
    d_act = lax.dot_general(d_out, w_down, (((1,), (1,)), ((), ())), preferred_element_type=jnp.float32)
    d_gate = (d_act * up_pre * sigmoid_gate * (1.0 + gate_pre * (1.0 - sigmoid_gate))).astype(jnp.bfloat16)
    d_up = (d_act * gate_pre * sigmoid_gate).astype(jnp.bfloat16)
    grad_gate = lax.dot_general(inputs, d_gate, (((0,), (0,)), ((), ())), preferred_element_type=jnp.float32)
    grad_up = lax.dot_general(inputs, d_up, (((0,), (0,)), ((), ())), preferred_element_type=jnp.float32)
    grad_down = lax.dot_general(activated, d_out, (((0,), (0,)), ((), ())), preferred_element_type=jnp.float32)
    return (grad_gate, grad_up, grad_down)

def lstm_step(features, recurrent_term, cell_old, input_weight, lstm_bias, context_weight):
    state_width = cell_old.shape[-1]
    lstm_in = jnp.dot(features, input_weight, precision=highest) + recurrent_term + lstm_bias
    in_gate = jax.nn.sigmoid(lstm_in[:, :state_width])
    forget_gate = jax.nn.sigmoid(lstm_in[:, state_width:2 * state_width])
    candidate = jnp.tanh(lstm_in[:, 2 * state_width:3 * state_width])
    out_gate = jax.nn.sigmoid(lstm_in[:, 3 * state_width:])
    cell_new = forget_gate * cell_old + in_gate * candidate
    hidden_new = out_gate * jnp.tanh(cell_new)
    context = jnp.dot(hidden_new, context_weight, precision=highest)
    return (hidden_new, cell_new, context)

def param_update(param, gradient, rms_param, rms_grad, context_row, mlp_weight):
    p_norm = param.astype(jnp.float32) / rms_param
    g_norm = gradient / rms_grad
    summed = jnp.zeros(param.shape, jnp.float32)
    for hidden_unit in range(mlp_weight.shape[1]):
        inner = mlp_weight[0, hidden_unit] * p_norm + mlp_weight[1, hidden_unit] * g_norm + context_row[hidden_unit]
        summed = summed + mlp_weight[2, hidden_unit] * jax.nn.relu(inner)
    update = jnp.exp(context_row[-1]) * summed
    new_param = (param.astype(jnp.float32) - rate_factor * rms_param * update).astype(jnp.bfloat16)
    return (update.astype(jnp.bfloat16), new_param)

def reference(tokens, targets, meta_tokens, meta_targets, gate_weight, up_weight, down_weight, task_step, hidden_state, cell_state, recurrent_weight, input_weight, lstm_bias, context_weight, mlp_weight):

    def one_task(operands):
        inputs, wanted, meta_in, meta_want, w_gate, w_up, w_down, step_now, hidden_old, cell_old = operands
        gate_pre, up_pre, sigmoid_gate, activated, output = block_forward(inputs, w_gate, w_up, w_down)
        d_out = (output - wanted.astype(jnp.float32)).astype(jnp.bfloat16)
        gradients = block_grads(inputs, w_down, gate_pre, up_pre, sigmoid_gate, activated, d_out)
        params = (w_gate, w_up, w_down)
        entries = float(D * FF)
        grad_sq = jnp.stack([jnp.sum(grad_piece * grad_piece) for grad_piece in gradients])
        param_sq = jnp.stack([jnp.sum(jnp.square(param_piece.astype(jnp.float32))) for param_piece in params])
        rms_grad = jnp.sqrt(grad_sq / entries + epsilon)
        rms_param = jnp.sqrt(param_sq / entries + epsilon)
        fraction = jnp.full((3,), step_now.astype(jnp.float32) / STEPS, jnp.float32)
        features = jnp.stack([jnp.log(rms_grad), jnp.log(rms_param), fraction], axis=1)
        recurrent_term = jnp.dot(hidden_old, recurrent_weight, precision=highest)
        hidden_new, cell_new, context = lstm_step(features, recurrent_term, cell_old, input_weight, lstm_bias, context_weight)
        results = [param_update(params[tensor_id], gradients[tensor_id], rms_param[tensor_id], rms_grad[tensor_id], context[tensor_id], mlp_weight) for tensor_id in range(3)]
        meta_out = block_forward(meta_in, results[0][1], results[1][1], results[2][1])[4]
        meta_part = 0.5 * jnp.sum(jnp.square(meta_out - meta_want.astype(jnp.float32))) / (TOK * D)
        return (results[0][0], results[1][0], results[2][0], hidden_new, cell_new, meta_part)
    gate_update, up_update, down_update, new_hidden, new_cell, meta_parts = lax.map(one_task, (tokens, targets, meta_tokens, meta_targets, gate_weight, up_weight, down_weight, task_step, hidden_state, cell_state))
    meta_loss = jnp.sum(meta_parts) / TASKS
    return (gate_update, up_update, down_update, new_hidden, new_cell, meta_loss)
```

```python
import functools

import jax
import jax.numpy as jnp
from jax import lax
from jax.experimental import pallas as pl
from jax.experimental.pallas import tpu as pltpu
from jax.sharding import Mesh
from jax.sharding import PartitionSpec as P


STEPS = 10000
X, Y, Z, SHARD = "task_0", "task_1", "task_2", "shard"
TASK = (X, Y, Z)

f32, bf16 = jnp.float32, jnp.bfloat16
highest = lax.Precision.HIGHEST
epsilon = 1e-06
rate_factor = 0.1
CHUNK = 256
MIB = 1 << 20


def dot(a, b):
    return jnp.dot(a, b, preferred_element_type=f32)


def dot_t(a, b):
    return lax.dot_general(a, b, (((1,), (1,)), ((), ())), preferred_element_type=f32)


def lane_sums(value):
    sums = jnp.sum(value, axis=0, keepdims=True)
    total = sums[:, :128]
    for start in range(128, sums.shape[1], 128):
        total = total + sums[:, start : start + 128]
    return total


def squares(value):
    value = value.astype(f32)
    return lane_sums(value * value)


def vmem(*shapes):
    return [pltpu.VMEM(shape, kind) for shape, kind in shapes]


IN_VMEM = pl.BlockSpec(memory_space=pltpu.VMEM)
IN_HBM = pl.BlockSpec(memory_space=pltpu.HBM)
IN_SMEM = pl.BlockSpec(memory_space=pltpu.SMEM)


def call(body, operands, specs, outs, out_specs, scratch=(), limit=8, flops=0):
    held = [pltpu.with_memory_space_constraint(a, pltpu.HBM) if spec is IN_HBM else a for a, spec in zip(operands, specs)]
    return pl.pallas_call(
        body,
        in_specs=specs,
        out_specs=out_specs,
        out_shape=outs,
        scratch_shapes=scratch,
        compiler_params=pltpu.CompilerParams(vmem_limit_bytes=limit * MIB),
        cost_estimate=pl.CostEstimate(flops=flops, transcendentals=0, bytes_accessed=0) if flops else None,
    )(*held)


def piece(j):
    return pl.ds(pl.multiple_of(j * CHUNK, CHUNK), CHUNK)


def forward_kernel(
    place_ref, x_hbm, wg_hbm, wu_hbm, wd_hbm, want_hbm, meta_hbm, meta_want_hbm,
    wg_ref, wu_ref, wd_ref, want_ref, meta_ref, meta_want_ref, out_ref, p_ref, q_ref, act_t_ref, x_t_ref, sq_ref,
    x_ref, sem_x, sem_w, sem_late,
):
    count = wg_ref.shape[1] // CHUNK
    half = meta_want_ref.shape[0]

    def weights(j):
        at = piece(j)
        return (
            pltpu.make_async_copy(wg_hbm.at[:, at], wg_ref.at[:, at], sem_w.at[0, j]),
            pltpu.make_async_copy(wu_hbm.at[:, at], wu_ref.at[:, at], sem_w.at[1, j]),
            pltpu.make_async_copy(wd_hbm.at[at, :], wd_ref.at[at, :], sem_w.at[2, j]),
        )

    mine = pl.ds(pl.multiple_of(place_ref[3] * half, half), half)
    late = (
        pltpu.make_async_copy(want_hbm, want_ref, sem_late.at[0]),
        pltpu.make_async_copy(meta_hbm, meta_ref, sem_late.at[1]),
        pltpu.make_async_copy(meta_want_hbm.at[mine, :], meta_want_ref, sem_late.at[2]),
    )
    first = pltpu.make_async_copy(x_hbm, x_ref, sem_x)
    first.start()
    for j in range(count):
        for copy in weights(j):
            copy.start()
    for copy in late:
        copy.start()
    sq_ref[...] = jnp.zeros_like(sq_ref)
    first.wait()

    def body(j, carry):
        at = piece(j)
        copies = weights(j)
        copies[0].wait()
        copies[1].wait()
        x = x_ref[...]
        gate = dot(x, wg_ref[:, at])
        up = dot(x, wu_ref[:, at])
        sig = jax.nn.sigmoid(gate)
        silu = gate * sig
        q_ref[:, at] = silu
        p_ref[:, at] = up * sig * (1.0 + gate * (1.0 - sig))
        act = (silu * up).astype(bf16)
        act_t_ref[at, :] = act.T
        copies[2].wait()
        part = dot(act, wd_ref[at, :])

        @pl.when(j == 0)
        def _():
            out_ref[...] = part
            x_t_ref[...] = x_ref[...].T

        @pl.when(j > 0)
        def _():
            out_ref[...] += part

        sq_ref[0:1, :] += squares(wg_ref[:, at])
        sq_ref[1:2, :] += squares(wu_ref[:, at])
        sq_ref[2:3, :] += squares(wd_ref[at, :])
        return carry

    lax.fori_loop(0, count, body, 0)
    for copy in late:
        copy.wait()


def forward(place, x, wg, wu, wd, want, meta, meta_want):
    tok, width = x.shape
    hid = wg.shape[1]
    outs = vmem(
        (wg.shape, bf16), (wu.shape, bf16), (wd.shape, bf16), (want.shape, bf16), (meta.shape, bf16),
        ((tok // 2, width), bf16), ((tok, width), f32), ((tok, hid), f32), ((tok, hid), f32),
        ((hid, tok), bf16), ((width, tok), bf16), ((8, 128), f32),
    )
    scratch = [
        pltpu.VMEM((tok, width), bf16),
        pltpu.SemaphoreType.DMA,
        pltpu.SemaphoreType.DMA((3, hid // CHUNK)),
        pltpu.SemaphoreType.DMA((3,)),
    ]
    return call(
        forward_kernel, (place, x, wg, wu, wd, want, meta, meta_want), [IN_SMEM] + [IN_HBM] * 7,
        outs, [IN_VMEM] * len(outs), scratch, 12, 6 * tok * width * hid,
    )


def backward_kernel(
    own_ref, recv_ref, want_ref, wd_ref, p_ref, q_ref, act_t_ref, x_t_ref, psq_ref, gg_ref, gu_ref, gd_ref, sq_ref, d_out_ref
):
    sq_ref[0:8, :] = jnp.zeros_like(psq_ref)
    sq_ref[8:16, :] = psq_ref[...]
    d_out_ref[...] = (own_ref[...] + recv_ref[...] - want_ref[...].astype(f32)).astype(bf16)

    def body(j, carry):
        at = piece(j)
        d_out = d_out_ref[...]
        d_act = dot_t(d_out, wd_ref[at, :])
        dg = (d_act * p_ref[:, at]).astype(bf16)
        du = (d_act * q_ref[:, at]).astype(bf16)
        x_t = x_t_ref[...]
        grad = dot(x_t, dg)
        gg_ref[:, at] = grad
        sq_ref[0:1, :] += squares(grad)
        grad = dot(x_t, du)
        gu_ref[:, at] = grad
        sq_ref[1:2, :] += squares(grad)
        grad = dot(act_t_ref[at, :], d_out)
        gd_ref[at, :] = grad
        sq_ref[2:3, :] += squares(grad)
        return carry

    lax.fori_loop(0, wd_ref.shape[0] // CHUNK, body, 0)


def backward(own, recv, want, wd, p, q, act_t, x_t, param_sq):
    tok, width = own.shape
    hid = wd.shape[0]
    outs = vmem(((width, hid), f32), ((width, hid), f32), ((hid, width), f32), ((16, 128), f32))
    return call(
        backward_kernel, (own, recv, want, wd, p, q, act_t, x_t, param_sq), [IN_VMEM] * 9,
        outs, [IN_VMEM] * 4, [pltpu.VMEM((tok, width), bf16)], 12, 8 * tok * width * hid,
    )


def recurrent_kernel(place_ref, own, h0, h1, h2, h3, r0, r1, r2, r3, o0, o1, o2, o3, stack):
    px, py, pz, core = place_ref[0], place_ref[1], place_ref[2], place_ref[3]
    state = own.shape[2]
    stack[...] = jnp.zeros_like(stack)
    for j in range(own.shape[0]):
        stack[j : j + 1, :] = jnp.where(core == 0, own[j], h0[j])
        stack[8 + j : 9 + j, :] = h1[j]
        stack[16 + j : 17 + j, :] = h2[j]
        stack[24 + j : 25 + j, :] = h3[j]
    shape = (state, 128)
    row = lax.broadcasted_iota(jnp.int32, shape, 0)
    col = lax.broadcasted_iota(jnp.int32, shape, 1)
    step, block, inner = col >> 4, (col >> 2) & 3, col & 3
    pick = (((px + block) & 3) << 7) + (((py + step) & 3) << 5) + (pz << 2) + inner
    chosen = (row == pick).astype(f32)
    hidden = jnp.dot(stack[...], chosen, precision=highest, preferred_element_type=f32)
    total = None
    for k, r_ref in enumerate((r0, r1, r2, r3)):
        term = jnp.dot(hidden[:, 16 * k : 16 * k + 16], r_ref[...], precision=highest, preferred_element_type=f32)
        total = term if total is None else total + term
    for k, out_ref in enumerate((o0, o1, o2, o3)):
        out_ref[...] = total[8 * k : 8 * k + 3]


def shifted(array, axis, shift):
    size = lax.axis_size(axis)
    return lax.ppermute(array, axis, [((i + shift) % size, i) for i in range(size)])


def swapped(array):
    return lax.ppermute(array, SHARD, [(0, 1), (1, 0)])


HOPS = ((None, 4), (1, -2), (-1, 3), (2, -3))


def hop(array, index, back):
    size = lax.axis_size(Z)
    pairs = []
    for core in range(2):
        by = HOPS[index][core]
        if by is None:
            continue
        for i in range(size):
            there = (i + by) % size
            pairs.append((there * 2 + core, i * 2 + core) if back else (i * 2 + core, there * 2 + core))
    return lax.ppermute(array, (Z, SHARD), pairs)


def line_kernel(r0, r1, r2, r3, out_ref):
    for k, r_ref in enumerate((r0, r1, r2, r3)):
        out_ref[4 * k : 4 * k + 4, :] = r_ref[...]


def sum_kernel(place_ref, own, m0, m1, m2, m3, out_ref):
    out_ref[...] = (jnp.where(place_ref[3] == 0, own[...], m0[...]) + m1[...]) + (m2[...] + m3[...])


def recurrent_line(weight):
    others = [shifted(weight, X, k) for k in (1, 2, 3)]
    shape = (4 * weight.shape[0], weight.shape[1])
    return call(line_kernel, (weight, *others), [IN_VMEM] * 4, vmem((shape, f32)), [IN_VMEM], (), 1, 1 << 16)[0]


def recurrent(hidden, hids, line, place):
    plane = [line] + [shifted(line, Y, k) for k in (1, 2, 3)]
    out = (hidden.shape[0], line.shape[1])
    parts = call(
        recurrent_kernel, (place, hidden, *hids, *plane), [IN_SMEM] + [IN_VMEM] * 9,
        vmem(*[(out, f32)] * 4), [IN_VMEM] * 4, [pltpu.VMEM((32, hidden.shape[2]), f32)], 4, 1 << 22,
    )
    moved = [hop(part, k, False) for k, part in enumerate(parts)]
    return call(
        sum_kernel, (place, parts[0], *moved), [IN_SMEM] + [IN_VMEM] * 5,
        vmem((out, f32)), [IN_VMEM], (), 1, 1 << 16,
    )[0]


def update_kernel(
    place_ref,
    mine_ref, theirs_ref, sq_ref, sq_recv_ref, in_w_ref, bias_ref, cell_ref, ctx_w_ref, mlp_ref,
    wg_ref, wu_ref, wd_ref, gg_ref, gu_ref, gd_ref, meta_ref,
    up_g_hbm, up_u_hbm, up_d_hbm, hidden_ref, new_cell_ref, send_ref, keep_ref,
    cell_old, table, table_s, order, sem, sem_out, out_g, out_u, out_d, new_g, new_u, new_d, acc,
):
    count = wg_ref.shape[1] // CHUNK
    units = mlp_ref.shape[1]
    entries = 2.0 * wg_ref.shape[0] * wg_ref.shape[1]

    sums = sq_ref[...] + sq_recv_ref[...]
    total = jnp.sum(sums, axis=1, keepdims=True)
    rms = jnp.sqrt(total / entries + epsilon)
    rms_g, rms_p = rms[0:3], rms[8:11]
    logs = jnp.log(rms)
    fraction = place_ref[4].astype(f32) / STEPS
    in_w = in_w_ref[...]
    lstm_in = (
        (logs[0:3] * in_w[0:1] + logs[8:11] * in_w[1:2] + fraction * in_w[2:3])
        + (mine_ref[...] + theirs_ref[...])
        + bias_ref[...]
    )
    width = cell_ref.shape[2]
    for j in range(3):
        cell_old[j : j + 1, :] = cell_ref[j]
    in_gate = jax.nn.sigmoid(lstm_in[:, :width])
    forget_gate = jax.nn.sigmoid(lstm_in[:, width : 2 * width])
    candidate = jnp.tanh(lstm_in[:, 2 * width : 3 * width])
    out_gate = jax.nn.sigmoid(lstm_in[:, 3 * width :])
    cell = forget_gate * cell_old[0:3, :] + in_gate * candidate
    hidden = out_gate * jnp.tanh(cell)
    for j in range(3):
        new_cell_ref[j] = cell[j : j + 1]
        hidden_ref[j] = hidden[j : j + 1]
    context = lax.dot_general(
        hidden, ctx_w_ref[...], (((1,), (1,)), ((), ())), precision=highest, preferred_element_type=f32
    )
    mlp = mlp_ref[...]
    out_w = mlp[2:3]
    table[0:3, :units] = out_w * mlp[0:1] / rms_p
    table[8:11, :units] = out_w * mlp[1:2] / rms_g
    table[16:19, :units] = -(out_w * context[:, :units])
    table[24:27, : units + 1] = jnp.exp(context)
    table[32:35, 0:1] = rate_factor * rms_p
    table[40:41, :units] = out_w
    copy = pltpu.make_async_copy(table, table_s, sem)
    copy.start()
    copy.wait()

    positive = jnp.int32(0)
    for k in range(units):
        positive = positive + (table_s[40, k] >= 0).astype(jnp.int32)
    above, below = jnp.int32(0), positive
    for k in range(units):
        is_above = table_s[40, k] >= 0
        spot = jnp.where(is_above, above, below)
        for j in range(3):
            for group in range(3):
                order[group * 12 + j * 4 + spot] = table_s[group * 8 + j, k]
        above = above + is_above.astype(jnp.int32)
        below = below + 1 - is_above.astype(jnp.int32)

    def change(which, j, w_ref, grad_ref, out_ref, new_ref, by_rows, strip):
        scale = table_s[24 + which, units]
        rate = table_s[32 + which, 0]
        a = [order[which * 4 + k] for k in range(units)]
        b = [order[12 + which * 4 + k] for k in range(units)]
        edge = [order[24 + which * 4 + k] for k in range(units)]
        offset = -functools.reduce(lambda s, e: s + e, edge)

        def variant(top):
            def body(i, carry):
                here = pl.ds(pl.multiple_of(i * strip, strip), strip)
                if by_rows:
                    there, lanes = pl.ds(pl.multiple_of(j * CHUNK + i * strip, strip), strip), slice(None)
                else:
                    there, lanes = here, piece(j)
                p = w_ref[there, lanes].astype(f32)
                g = grad_ref[there, lanes]
                total = None
                for k in range(units):
                    term = a[k] * p + b[k] * g
                    term = jnp.maximum(term, edge[k]) if k < top else jnp.minimum(term, edge[k])
                    total = term if total is None else total + term
                upd = scale * (total + offset)
                out_ref[there, lanes] = upd.astype(bf16)
                new_ref[here, :] = (p - rate * upd).astype(bf16)
                return carry

            lax.fori_loop(0, new_ref.shape[0] // strip, body, 0)

        for top in range(units + 1):
            pl.when(positive == top)(functools.partial(variant, top))

    def results(j):
        at = piece(j)
        return (
            pltpu.make_async_copy(out_g.at[:, at], up_g_hbm.at[:, at], sem_out.at[0, j]),
            pltpu.make_async_copy(out_u.at[:, at], up_u_hbm.at[:, at], sem_out.at[1, j]),
            pltpu.make_async_copy(out_d.at[at, :], up_d_hbm.at[at, :], sem_out.at[2, j]),
        )

    def body(j, carry):
        copies = results(j)
        change(0, j, wg_ref, gg_ref, out_g, new_g, False, STRIP)
        copies[0].start()
        change(1, j, wu_ref, gu_ref, out_u, new_u, False, STRIP)
        copies[1].start()
        change(2, j, wd_ref, gd_ref, out_d, new_d, True, STRIP // 4)
        copies[2].start()
        meta = meta_ref[...]
        gate = dot(meta, new_g[...])
        up = dot(meta, new_u[...])
        act = (gate * jax.nn.sigmoid(gate) * up).astype(bf16)
        part = dot(act, new_d[...])

        @pl.when(j == 0)
        def _():
            acc[...] = part

        @pl.when(j > 0)
        def _():
            acc[...] += part

        return carry

    lax.fori_loop(0, count, body, 0)
    half = acc.shape[0] // 2
    core = place_ref[3]
    keep_ref[...] = acc[pl.ds(pl.multiple_of(core * half, half), half), :]
    send_ref[...] = acc[pl.ds(pl.multiple_of((1 - core) * half, half), half), :]
    for j in range(count):
        for copy in results(j):
            copy.wait()


STRIP = 64


def update(place, mine, theirs, sums, sums_recv, in_w, bias, cell, ctx_w, mlp, wg, wu, wd, gg, gu, gd, meta):
    tok, width = meta.shape
    hid = wg.shape[1]
    outs = [pltpu.HBM(wg.shape, bf16), pltpu.HBM(wu.shape, bf16), pltpu.HBM(wd.shape, bf16)]
    outs += vmem((cell.shape, f32), (cell.shape, f32), ((tok // 2, width), f32), ((tok // 2, width), f32))
    scratch = [
        pltpu.VMEM((8, cell.shape[2]), f32),
        pltpu.VMEM((48, 128), f32),
        pltpu.SMEM((48, 128), f32),
        pltpu.SMEM((48,), f32),
        pltpu.SemaphoreType.DMA,
        pltpu.SemaphoreType.DMA((3, hid // CHUNK)),
        pltpu.VMEM(wg.shape, bf16),
        pltpu.VMEM(wu.shape, bf16),
        pltpu.VMEM(wd.shape, bf16),
        pltpu.VMEM((width, CHUNK), bf16),
        pltpu.VMEM((width, CHUNK), bf16),
        pltpu.VMEM((CHUNK, width), bf16),
        pltpu.VMEM((tok, width), f32),
    ]
    operands = (place, mine, theirs, sums, sums_recv, in_w, bias, cell, ctx_w, mlp, wg, wu, wd, gg, gu, gd, meta)
    return call(
        update_kernel, operands, [IN_SMEM] + [IN_VMEM] * 16,
        outs, [IN_HBM] * 3 + [IN_VMEM] * 4, scratch, 20, 6 * tok * width * hid,
    )


def loss_kernel(scale, keep_ref, recv_ref, want_ref, out_ref):
    error = keep_ref[...] + recv_ref[...] - want_ref[...].astype(f32)
    total = jnp.sum(jnp.sum(error * error, axis=0, keepdims=True), axis=1, keepdims=True)
    out_ref[...] = jnp.broadcast_to(scale * total, out_ref.shape)


def loss_part(keep, recv, want, count):
    scale = 0.25 / (want.shape[0] * want.shape[1]) / count
    return call(
        functools.partial(loss_kernel, scale), (keep, recv, want), [IN_VMEM] * 3,
        vmem(((1, 128), f32)), [IN_VMEM], (), 8,
    )[0]


def local(
    tokens, targets, meta_tokens, meta_targets, gate_weight, up_weight, down_weight, task_step,
    hidden_state, cell_state, recurrent_weight, input_weight, lstm_bias, context_weight, mlp_weight,
):
    core = lax.axis_index(SHARD)
    place = jnp.stack([lax.axis_index(X), lax.axis_index(Y), lax.axis_index(Z), core, task_step[0]]).astype(jnp.int32)
    hidden = hidden_state.transpose(1, 0, 2)
    line = recurrent_line(recurrent_weight)
    hids = [hop(hidden, k, True) for k in range(4)]
    wg, wu, wd, want, meta, meta_want, own, p, q, act_t, x_t, param_sq = forward(
        place, tokens[0], gate_weight[0], up_weight[0], down_weight[0], targets[0], meta_tokens[0], meta_targets[0]
    )
    recv = swapped(own)
    mine = recurrent(hidden, hids, line, place)
    gg, gu, gd, sums = backward(own, recv, want, wd, p, q, act_t, x_t, param_sq)
    up_g, up_u, up_d, new_hidden, new_cell, send, keep = update(
        place, mine, swapped(mine), sums, swapped(sums), input_weight, lstm_bias[None], cell_state.transpose(1, 0, 2),
        context_weight.T, mlp_weight, wg, wu, wd, gg, gu, gd, meta,
    )
    count = lax.axis_size(TASK)
    part = loss_part(keep, swapped(send), meta_want, count)
    part = part + swapped(part)
    everyone = lax.all_to_all(part.reshape(count), TASK, 0, 0, tiled=True)
    meta_loss = jnp.sum(everyone)
    return (
        up_g[None], up_u[None], up_d[None], new_hidden.transpose(1, 0, 2), new_cell.transpose(1, 0, 2), meta_loss
    )


def solution(mesh):
    finer = Mesh(mesh.devices.reshape(4, 4, 8, mesh.shape["shard"]), (X, Y, Z, SHARD))
    return jax.shard_map(
        local,
        mesh=finer,
        in_specs=(
            P(TASK, None, None), P(TASK, None, None), P(TASK, None, None), P(TASK, None, None),
            P(TASK, None, "shard"), P(TASK, None, "shard"), P(TASK, "shard", None), P(TASK),
            P(TASK, None, None), P(TASK, None, None), P(TASK, None), P(), P(), P(), P(),
        ),
        out_specs=(
            P(TASK, None, "shard"), P(TASK, None, "shard"), P(TASK, "shard", None),
            P(TASK, None, None), P(TASK, None, None), P(),
        ),
        check_vma=False,
    )
```

```python
import functools

import jax
import jax.numpy as jnp
from jax import lax
from jax.experimental import pallas as pl
from jax.experimental.pallas import tpu as pltpu
from jax.sharding import Mesh
from jax.sharding import PartitionSpec as P


STEPS = 10000
X, Y, Z, SHARD = "task_0", "task_1", "task_2", "shard"
TASK = (X, Y, Z)

f32, bf16 = jnp.float32, jnp.bfloat16
highest = lax.Precision.HIGHEST
epsilon = 1e-06
rate_factor = 0.1
CHUNK = 256
MIB = 1 << 20


def dot(a, b):
    return jnp.dot(a, b, preferred_element_type=f32)


def dot_t(a, b):
    return lax.dot_general(a, b, (((1,), (1,)), ((), ())), preferred_element_type=f32)


def lane_sums(value):
    sums = jnp.sum(value, axis=0, keepdims=True)
    total = sums[:, :128]
    for start in range(128, sums.shape[1], 128):
        total = total + sums[:, start : start + 128]
    return total


def squares(value):
    value = value.astype(f32)
    return lane_sums(value * value)


def vmem(*shapes):
    return [pltpu.VMEM(shape, kind) for shape, kind in shapes]


IN_VMEM = pl.BlockSpec(memory_space=pltpu.VMEM)
IN_HBM = pl.BlockSpec(memory_space=pltpu.HBM)
IN_SMEM = pl.BlockSpec(memory_space=pltpu.SMEM)


def call(body, operands, specs, outs, out_specs, scratch=(), limit=8, flops=0):
    held = [pltpu.with_memory_space_constraint(a, pltpu.HBM) if spec is IN_HBM else a for a, spec in zip(operands, specs)]
    return pl.pallas_call(
        body,
        in_specs=specs,
        out_specs=out_specs,
        out_shape=outs,
        scratch_shapes=scratch,
        compiler_params=pltpu.CompilerParams(vmem_limit_bytes=limit * MIB),
        cost_estimate=pl.CostEstimate(flops=flops, transcendentals=0, bytes_accessed=0) if flops else None,
    )(*held)


def piece(j):
    return pl.ds(pl.multiple_of(j * CHUNK, CHUNK), CHUNK)


def forward_kernel(x_ref, wg_ref, wu_ref, wd_ref, out_ref, p_ref, q_ref, act_t_ref, x_t_ref, sq_ref):
    sq_ref[...] = jnp.zeros_like(sq_ref)

    def body(j, carry):
        at = piece(j)
        x = x_ref[...]
        gate = dot(x, wg_ref[:, at])
        up = dot(x, wu_ref[:, at])
        sig = jax.nn.sigmoid(gate)
        silu = gate * sig
        q_ref[:, at] = silu
        p_ref[:, at] = up * sig * (1.0 + gate * (1.0 - sig))
        act = (silu * up).astype(bf16)
        act_t_ref[at, :] = act.T
        part = dot(act, wd_ref[at, :])

        @pl.when(j == 0)
        def _():
            out_ref[...] = part
            x_t_ref[...] = x_ref[...].T

        @pl.when(j > 0)
        def _():
            out_ref[...] += part

        sq_ref[0:1, :] += squares(wg_ref[:, at])
        sq_ref[1:2, :] += squares(wu_ref[:, at])
        sq_ref[2:3, :] += squares(wd_ref[at, :])
        return carry

    lax.fori_loop(0, wg_ref.shape[1] // CHUNK, body, 0)


def forward(x, wg, wu, wd):
    tok, width = x.shape
    hid = wg.shape[1]
    outs = vmem(
        ((tok, width), f32), ((tok, hid), f32), ((tok, hid), f32), ((hid, tok), bf16), ((width, tok), bf16), ((8, 128), f32),
    )
    return call(
        forward_kernel, (x, wg, wu, wd), [IN_VMEM] * 4,
        outs, [IN_VMEM] * len(outs), (), 8, 6 * tok * width * hid,
    )


def backward_kernel(
    own_ref, recv_ref, want_ref, wd_ref, p_ref, q_ref, act_t_ref, x_t_ref, psq_ref, gg_ref, gu_ref, gd_ref, sq_ref, d_out_ref
):
    sq_ref[0:8, :] = jnp.zeros_like(psq_ref)
    sq_ref[8:16, :] = psq_ref[...]
    d_out_ref[...] = (own_ref[...] + recv_ref[...] - want_ref[...].astype(f32)).astype(bf16)

    def body(j, carry):
        at = piece(j)
        d_out = d_out_ref[...]
        d_act = dot_t(d_out, wd_ref[at, :])
        dg = (d_act * p_ref[:, at]).astype(bf16)
        du = (d_act * q_ref[:, at]).astype(bf16)
        x_t = x_t_ref[...]
        grad = dot(x_t, dg)
        gg_ref[:, at] = grad
        sq_ref[0:1, :] += squares(grad)
        grad = dot(x_t, du)
        gu_ref[:, at] = grad
        sq_ref[1:2, :] += squares(grad)
        grad = dot(act_t_ref[at, :], d_out)
        gd_ref[at, :] = grad
        sq_ref[2:3, :] += squares(grad)
        return carry

    lax.fori_loop(0, wd_ref.shape[0] // CHUNK, body, 0)


def backward(own, recv, want, wd, p, q, act_t, x_t, param_sq):
    tok, width = own.shape
    hid = wd.shape[0]
    outs = vmem(((width, hid), f32), ((width, hid), f32), ((hid, width), f32), ((16, 128), f32))
    return call(
        backward_kernel, (own, recv, want, wd, p, q, act_t, x_t, param_sq), [IN_VMEM] * 9,
        outs, [IN_VMEM] * 4, [pltpu.VMEM((tok, width), bf16)], 12, 8 * tok * width * hid,
    )


def recurrent_kernel(place_ref, own, h0, h1, h2, h3, r0, r1, r2, r3, o0, o1, o2, o3, stack):
    px, py, pz, core = place_ref[0], place_ref[1], place_ref[2], place_ref[3]
    state = own.shape[2]
    stack[...] = jnp.zeros_like(stack)
    for j in range(own.shape[0]):
        stack[j : j + 1, :] = jnp.where(core == 0, own[j], h0[j])
        stack[8 + j : 9 + j, :] = h1[j]
        stack[16 + j : 17 + j, :] = h2[j]
        stack[24 + j : 25 + j, :] = h3[j]
    shape = (state, 128)
    row = lax.broadcasted_iota(jnp.int32, shape, 0)
    col = lax.broadcasted_iota(jnp.int32, shape, 1)
    step, block, inner = col >> 4, (col >> 2) & 3, col & 3
    pick = (((px + block) & 3) << 7) + (((py + step) & 3) << 5) + (pz << 2) + inner
    chosen = (row == pick).astype(f32)
    hidden = jnp.dot(stack[...], chosen, precision=highest, preferred_element_type=f32)
    total = None
    for k, r_ref in enumerate((r0, r1, r2, r3)):
        term = jnp.dot(hidden[:, 16 * k : 16 * k + 16], r_ref[...], precision=highest, preferred_element_type=f32)
        total = term if total is None else total + term
    for k, out_ref in enumerate((o0, o1, o2, o3)):
        out_ref[...] = total[8 * k : 8 * k + 3]


def shifted(array, axis, shift):
    size = lax.axis_size(axis)
    return lax.ppermute(array, axis, [((i + shift) % size, i) for i in range(size)])


def swapped(array):
    return lax.ppermute(array, SHARD, [(0, 1), (1, 0)])


HOPS = ((None, -1), (1, 2), (3, -2), (4, -3))


def hop(array, index, back):
    size = lax.axis_size(Z)
    pairs = []
    for core in range(2):
        by = HOPS[index][core]
        if by is None:
            continue
        for i in range(size):
            there = (i + by) % size
            pairs.append((there * 2 + core, i * 2 + core) if back else (i * 2 + core, there * 2 + core))
    return lax.ppermute(array, (Z, SHARD), pairs)


def first_kernel(place_ref, hidden_hbm, weight_hbm, hidden_ref, weight_ref, sems):
    copies = (
        pltpu.make_async_copy(weight_hbm, weight_ref, sems.at[0]),
        pltpu.make_async_copy(hidden_hbm, hidden_ref, sems.at[1]),
    )
    for copy in copies:
        copy.start()
    for copy in copies:
        copy.wait()


def brought(place, hidden, weight):
    return call(
        first_kernel, (place, hidden, weight), [IN_SMEM] + [IN_HBM] * 2, vmem((hidden.shape, f32), (weight.shape, f32)),
        [IN_VMEM] * 2, [pltpu.SemaphoreType.DMA((2,))], 1, 100_000_000_000,
    )


def line_kernel(r0, r1, r2, r3, out_ref):
    for k, r_ref in enumerate((r0, r1, r2, r3)):
        out_ref[4 * k : 4 * k + 4, :] = r_ref[...]


def sum_kernel(place_ref, own, m0, m1, m2, m3, out_ref):
    out_ref[...] = (jnp.where(place_ref[3] == 0, own[...], m0[...]) + m1[...]) + (m2[...] + m3[...])


def recurrent_line(weight):
    others = [shifted(weight, X, k) for k in (1, 2, 3)]
    shape = (4 * weight.shape[0], weight.shape[1])
    return call(line_kernel, (weight, *others), [IN_VMEM] * 4, vmem((shape, f32)), [IN_VMEM], (), 1, 1 << 16)[0]


def recurrent(hidden, hids, line, place):
    plane = [line] + [shifted(line, Y, k) for k in (1, 2, 3)]
    out = (hidden.shape[0], line.shape[1])
    parts = call(
        recurrent_kernel, (place, hidden, *hids, *plane), [IN_SMEM] + [IN_VMEM] * 9,
        vmem(*[(out, f32)] * 4), [IN_VMEM] * 4, [pltpu.VMEM((32, hidden.shape[2]), f32)], 4, 1 << 22,
    )
    moved = [hop(part, k, False) for k, part in enumerate(parts)]
    return call(
        sum_kernel, (place, parts[0], *moved), [IN_SMEM] + [IN_VMEM] * 5,
        vmem((out, f32)), [IN_VMEM], (), 1, 1 << 16,
    )[0]


def update_kernel(
    place_ref,
    mine_ref, theirs_ref, sq_ref, sq_recv_ref, in_w_ref, bias_ref, cell_ref, ctx_w_ref, mlp_ref,
    wg_ref, wu_ref, wd_ref, gg_ref, gu_ref, gd_ref, meta_ref,
    up_g_hbm, up_u_hbm, up_d_hbm, hidden_ref, new_cell_ref, send_ref, keep_ref,
    cell_old, table, table_s, order, sem, sem_out, out_g, out_u, out_d, new_g, new_u, new_d, acc,
):
    count = wg_ref.shape[1] // CHUNK
    units = mlp_ref.shape[1]
    entries = 2.0 * wg_ref.shape[0] * wg_ref.shape[1]

    sums = sq_ref[...] + sq_recv_ref[...]
    total = jnp.sum(sums, axis=1, keepdims=True)
    rms = jnp.sqrt(total / entries + epsilon)
    rms_g, rms_p = rms[0:3], rms[8:11]
    logs = jnp.log(rms)
    fraction = place_ref[4].astype(f32) / STEPS
    in_w = in_w_ref[...]
    lstm_in = (
        (logs[0:3] * in_w[0:1] + logs[8:11] * in_w[1:2] + fraction * in_w[2:3])
        + (mine_ref[...] + theirs_ref[...])
        + bias_ref[...]
    )
    width = cell_ref.shape[2]
    for j in range(3):
        cell_old[j : j + 1, :] = cell_ref[j]
    in_gate = jax.nn.sigmoid(lstm_in[:, :width])
    forget_gate = jax.nn.sigmoid(lstm_in[:, width : 2 * width])
    candidate = jnp.tanh(lstm_in[:, 2 * width : 3 * width])
    out_gate = jax.nn.sigmoid(lstm_in[:, 3 * width :])
    cell = forget_gate * cell_old[0:3, :] + in_gate * candidate
    hidden = out_gate * jnp.tanh(cell)
    for j in range(3):
        new_cell_ref[j] = cell[j : j + 1]
        hidden_ref[j] = hidden[j : j + 1]
    context = lax.dot_general(
        hidden, ctx_w_ref[...], (((1,), (1,)), ((), ())), precision=highest, preferred_element_type=f32
    )
    mlp = mlp_ref[...]
    out_w = mlp[2:3]
    table[0:3, :units] = out_w * mlp[0:1] / rms_p
    table[8:11, :units] = out_w * mlp[1:2] / rms_g
    table[16:19, :units] = -(out_w * context[:, :units])
    table[24:27, : units + 1] = jnp.exp(context)
    table[32:35, 0:1] = rate_factor * rms_p
    table[40:41, :units] = out_w
    copy = pltpu.make_async_copy(table, table_s, sem)
    copy.start()
    copy.wait()

    positive = jnp.int32(0)
    for k in range(units):
        positive = positive + (table_s[40, k] >= 0).astype(jnp.int32)
    above, below = jnp.int32(0), positive
    for k in range(units):
        is_above = table_s[40, k] >= 0
        spot = jnp.where(is_above, above, below)
        for j in range(3):
            for group in range(3):
                order[group * 12 + j * 4 + spot] = table_s[group * 8 + j, k]
        above = above + is_above.astype(jnp.int32)
        below = below + 1 - is_above.astype(jnp.int32)

    def change(which, j, w_ref, grad_ref, out_ref, new_ref, by_rows, strip):
        scale = table_s[24 + which, units]
        rate = table_s[32 + which, 0]
        a = [order[which * 4 + k] for k in range(units)]
        b = [order[12 + which * 4 + k] for k in range(units)]
        edge = [order[24 + which * 4 + k] for k in range(units)]
        offset = -functools.reduce(lambda s, e: s + e, edge)

        def variant(top):
            def body(i, carry):
                here = pl.ds(pl.multiple_of(i * strip, strip), strip)
                if by_rows:
                    there, lanes = pl.ds(pl.multiple_of(j * CHUNK + i * strip, strip), strip), slice(None)
                else:
                    there, lanes = here, piece(j)
                p = w_ref[there, lanes].astype(f32)
                g = grad_ref[there, lanes]
                total = None
                for k in range(units):
                    term = a[k] * p + b[k] * g
                    term = jnp.maximum(term, edge[k]) if k < top else jnp.minimum(term, edge[k])
                    total = term if total is None else total + term
                upd = scale * (total + offset)
                out_ref[there, lanes] = upd.astype(bf16)
                new_ref[here, :] = (p - rate * upd).astype(bf16)
                return carry

            lax.fori_loop(0, new_ref.shape[0] // strip, body, 0)

        for top in range(units + 1):
            pl.when(positive == top)(functools.partial(variant, top))

    def results(j):
        at = piece(j)
        return (
            pltpu.make_async_copy(out_g.at[:, at], up_g_hbm.at[:, at], sem_out.at[0, j]),
            pltpu.make_async_copy(out_u.at[:, at], up_u_hbm.at[:, at], sem_out.at[1, j]),
            pltpu.make_async_copy(out_d.at[at, :], up_d_hbm.at[at, :], sem_out.at[2, j]),
        )

    def body(j, carry):
        copies = results(j)
        change(0, j, wg_ref, gg_ref, out_g, new_g, False, STRIP)
        copies[0].start()
        change(1, j, wu_ref, gu_ref, out_u, new_u, False, STRIP)
        copies[1].start()
        change(2, j, wd_ref, gd_ref, out_d, new_d, True, STRIP // 4)
        copies[2].start()
        meta = meta_ref[...]
        gate = dot(meta, new_g[...])
        up = dot(meta, new_u[...])
        act = (gate * jax.nn.sigmoid(gate) * up).astype(bf16)
        part = dot(act, new_d[...])

        @pl.when(j == 0)
        def _():
            acc[...] = part

        @pl.when(j > 0)
        def _():
            acc[...] += part

        return carry

    lax.fori_loop(0, count, body, 0)
    half = acc.shape[0] // 2
    core = place_ref[3]
    keep_ref[...] = acc[pl.ds(pl.multiple_of(core * half, half), half), :]
    send_ref[...] = acc[pl.ds(pl.multiple_of((1 - core) * half, half), half), :]
    for j in range(count):
        for copy in results(j):
            copy.wait()


STRIP = 64


def update(place, mine, theirs, sums, sums_recv, in_w, bias, cell, ctx_w, mlp, wg, wu, wd, gg, gu, gd, meta):
    tok, width = meta.shape
    hid = wg.shape[1]
    outs = [pltpu.HBM(wg.shape, bf16), pltpu.HBM(wu.shape, bf16), pltpu.HBM(wd.shape, bf16)]
    outs += vmem((cell.shape, f32), (cell.shape, f32), ((tok // 2, width), f32), ((tok // 2, width), f32))
    scratch = [
        pltpu.VMEM((8, cell.shape[2]), f32),
        pltpu.VMEM((48, 128), f32),
        pltpu.SMEM((48, 128), f32),
        pltpu.SMEM((48,), f32),
        pltpu.SemaphoreType.DMA,
        pltpu.SemaphoreType.DMA((3, hid // CHUNK)),
        pltpu.VMEM(wg.shape, bf16),
        pltpu.VMEM(wu.shape, bf16),
        pltpu.VMEM(wd.shape, bf16),
        pltpu.VMEM((width, CHUNK), bf16),
        pltpu.VMEM((width, CHUNK), bf16),
        pltpu.VMEM((CHUNK, width), bf16),
        pltpu.VMEM((tok, width), f32),
    ]
    operands = (place, mine, theirs, sums, sums_recv, in_w, bias, cell, ctx_w, mlp, wg, wu, wd, gg, gu, gd, meta)
    return call(
        update_kernel, operands, [IN_SMEM] + [IN_VMEM] * 16,
        outs, [IN_HBM] * 3 + [IN_VMEM] * 4, scratch, 20, 6 * tok * width * hid,
    )


def loss_kernel(scale, place_ref, keep_ref, recv_ref, want_ref, out_ref):
    half = keep_ref.shape[0]
    mine = pl.ds(pl.multiple_of(place_ref[3] * half, half), half)
    error = keep_ref[...] + recv_ref[...] - want_ref[mine, :].astype(f32)
    total = jnp.sum(jnp.sum(error * error, axis=0, keepdims=True), axis=1, keepdims=True)
    out_ref[...] = jnp.broadcast_to(scale * total, out_ref.shape)


def loss_part(place, keep, recv, want, count):
    scale = 0.5 / (want.shape[0] * want.shape[1]) / count
    return call(
        functools.partial(loss_kernel, scale), (place, keep, recv, want), [IN_SMEM] + [IN_VMEM] * 3,
        vmem(((1, 128), f32)), [IN_VMEM], (), 8,
    )[0]


def local(
    tokens, targets, meta_tokens, meta_targets, gate_weight, up_weight, down_weight, task_step,
    hidden_state, cell_state, recurrent_weight, input_weight, lstm_bias, context_weight, mlp_weight,
):
    core = lax.axis_index(SHARD)
    place = jnp.stack([lax.axis_index(X), lax.axis_index(Y), lax.axis_index(Z), core, task_step[0]]).astype(jnp.int32)
    hidden, weight = brought(place, hidden_state.transpose(1, 0, 2), recurrent_weight)
    line = recurrent_line(weight)
    hids = [hop(hidden, k, True) for k in range(4)]
    wg, wu, wd = gate_weight[0], up_weight[0], down_weight[0]
    own, p, q, act_t, x_t, param_sq = forward(tokens[0], wg, wu, wd)
    recv = swapped(own)
    mine = recurrent(hidden, hids, line, place)
    gg, gu, gd, sums = backward(own, recv, targets[0], wd, p, q, act_t, x_t, param_sq)
    up_g, up_u, up_d, new_hidden, new_cell, send, keep = update(
        place, mine, swapped(mine), sums, swapped(sums), input_weight, lstm_bias[None], cell_state.transpose(1, 0, 2),
        context_weight.T, mlp_weight, wg, wu, wd, gg, gu, gd, meta_tokens[0],
    )
    count = lax.axis_size(TASK)
    part = loss_part(place, keep, swapped(send), meta_targets[0], count)
    part = part + swapped(part)
    everyone = lax.all_to_all(part.reshape(count), TASK, 0, 0, tiled=True)
    meta_loss = jnp.sum(everyone)
    return (
        up_g[None], up_u[None], up_d[None], new_hidden.transpose(1, 0, 2), new_cell.transpose(1, 0, 2), meta_loss
    )


def solution(mesh):
    finer = Mesh(mesh.devices.reshape(4, 4, 8, mesh.shape["shard"]), (X, Y, Z, SHARD))
    return jax.shard_map(
        local,
        mesh=finer,
        in_specs=(
            P(TASK, None, None), P(TASK, None, None), P(TASK, None, None), P(TASK, None, None),
            P(TASK, None, "shard"), P(TASK, None, "shard"), P(TASK, "shard", None), P(TASK),
            P(TASK, None, None), P(TASK, None, None), P(TASK, None), P(), P(), P(), P(),
        ),
        out_specs=(
            P(TASK, None, "shard"), P(TASK, None, "shard"), P(TASK, "shard", None),
            P(TASK, None, None), P(TASK, None, None), P(),
        ),
        check_vma=False,
    )
```

```python
import functools

import jax
import jax.numpy as jnp
from jax import lax
from jax.experimental import pallas as pl
from jax.experimental.pallas import tpu as pltpu
from jax.sharding import Mesh
from jax.sharding import PartitionSpec as P


STEPS = 10000
X, Y, Z, SHARD = "task_0", "task_1", "task_2", "shard"
TASK = (X, Y, Z)

f32, bf16 = jnp.float32, jnp.bfloat16
highest = lax.Precision.HIGHEST
epsilon = 1e-06
rate_factor = 0.1
CHUNK = 256
MIB = 1 << 20


def dot(a, b):
    return jnp.dot(a, b, preferred_element_type=f32)


def dot_t(a, b):
    return lax.dot_general(a, b, (((1,), (1,)), ((), ())), preferred_element_type=f32)


def lane_sums(value):
    sums = jnp.sum(value, axis=0, keepdims=True)
    total = sums[:, :128]
    for start in range(128, sums.shape[1], 128):
        total = total + sums[:, start : start + 128]
    return total


def squares(value):
    value = value.astype(f32)
    return lane_sums(value * value)


def vmem(*shapes):
    return [pltpu.VMEM(shape, kind) for shape, kind in shapes]


IN_VMEM = pl.BlockSpec(memory_space=pltpu.VMEM)
IN_HBM = pl.BlockSpec(memory_space=pltpu.HBM)
IN_SMEM = pl.BlockSpec(memory_space=pltpu.SMEM)


def call(body, operands, specs, outs, out_specs, scratch=(), limit=8, flops=0):
    held = [pltpu.with_memory_space_constraint(a, pltpu.HBM) if spec is IN_HBM else a for a, spec in zip(operands, specs)]
    return pl.pallas_call(
        body,
        in_specs=specs,
        out_specs=out_specs,
        out_shape=outs,
        scratch_shapes=scratch,
        compiler_params=pltpu.CompilerParams(vmem_limit_bytes=limit * MIB),
        cost_estimate=pl.CostEstimate(flops=flops, transcendentals=0, bytes_accessed=0) if flops else None,
    )(*held)


def piece(j):
    return pl.ds(pl.multiple_of(j * CHUNK, CHUNK), CHUNK)


def forward_kernel(x_ref, wg_ref, wu_ref, wd_ref, out_ref, p_ref, q_ref, act_t_ref, x_t_ref, sq_ref):
    sq_ref[...] = jnp.zeros_like(sq_ref)

    def body(j, carry):
        at = piece(j)
        x = x_ref[...]
        gate = dot(x, wg_ref[:, at])
        up = dot(x, wu_ref[:, at])
        sig = jax.nn.sigmoid(gate)
        silu = gate * sig
        q_ref[:, at] = silu
        p_ref[:, at] = up * sig * (1.0 + gate * (1.0 - sig))
        act = (silu * up).astype(bf16)
        act_t_ref[at, :] = act.T
        part = dot(act, wd_ref[at, :])

        @pl.when(j == 0)
        def _():
            out_ref[...] = part
            x_t_ref[...] = x_ref[...].T

        @pl.when(j > 0)
        def _():
            out_ref[...] += part

        sq_ref[0:1, :] += squares(wg_ref[:, at])
        sq_ref[1:2, :] += squares(wu_ref[:, at])
        sq_ref[2:3, :] += squares(wd_ref[at, :])
        return carry

    lax.fori_loop(0, wg_ref.shape[1] // CHUNK, body, 0)


def forward(x, wg, wu, wd):
    tok, width = x.shape
    hid = wg.shape[1]
    outs = vmem(
        ((tok, width), f32), ((tok, hid), f32), ((tok, hid), f32), ((hid, tok), bf16), ((width, tok), bf16), ((8, 128), f32),
    )
    return call(
        forward_kernel, (x, wg, wu, wd), [IN_VMEM] * 4,
        outs, [IN_VMEM] * len(outs), (), 8, 6 * tok * width * hid,
    )


def backward_kernel(
    own_ref, recv_ref, want_ref, wd_ref, p_ref, q_ref, act_t_ref, x_t_ref, psq_ref, gg_ref, gu_ref, gd_ref, sq_ref, d_out_ref
):
    sq_ref[0:8, :] = jnp.zeros_like(psq_ref)
    sq_ref[8:16, :] = psq_ref[...]
    d_out_ref[...] = (own_ref[...] + recv_ref[...] - want_ref[...].astype(f32)).astype(bf16)

    def body(j, carry):
        at = piece(j)
        d_out = d_out_ref[...]
        d_act = dot_t(d_out, wd_ref[at, :])
        dg = (d_act * p_ref[:, at]).astype(bf16)
        du = (d_act * q_ref[:, at]).astype(bf16)
        x_t = x_t_ref[...]
        grad = dot(x_t, dg)
        gg_ref[:, at] = grad
        sq_ref[0:1, :] += squares(grad)
        grad = dot(x_t, du)
        gu_ref[:, at] = grad
        sq_ref[1:2, :] += squares(grad)
        grad = dot(act_t_ref[at, :], d_out)
        gd_ref[at, :] = grad
        sq_ref[2:3, :] += squares(grad)
        return carry

    lax.fori_loop(0, wd_ref.shape[0] // CHUNK, body, 0)


def backward(own, recv, want, wd, p, q, act_t, x_t, param_sq):
    tok, width = own.shape
    hid = wd.shape[0]
    outs = vmem(((width, hid), f32), ((width, hid), f32), ((hid, width), f32), ((16, 128), f32))
    return call(
        backward_kernel, (own, recv, want, wd, p, q, act_t, x_t, param_sq), [IN_VMEM] * 9,
        outs, [IN_VMEM] * 4, [pltpu.VMEM((tok, width), bf16)], 12, 8 * tok * width * hid,
    )


def recurrent_kernel(info_ref, own, h1, h2, h3, h4, across, r0, r1, r2, r3, o0, o1, o2, o3, stack):
    px, py, pz, core = (info_ref[k : k + 1, 0:1] for k in range(4))
    state = own.shape[2]
    stack[...] = jnp.zeros_like(stack)
    for j in range(own.shape[0]):
        stack[j : j + 1, :] = jnp.where(core == 0, own[j], h1[j])
        stack[8 + j : 9 + j, :] = jnp.where(core == 0, h1[j], across[j])
        stack[16 + j : 17 + j, :] = jnp.where(core == 0, h3[j], h2[j])
        stack[24 + j : 25 + j, :] = jnp.where(core == 0, h4[j], h3[j])
    shape = (state, 128)
    row = lax.broadcasted_iota(jnp.int32, shape, 0)
    col = lax.broadcasted_iota(jnp.int32, shape, 1)
    step, block, inner = col >> 4, (col >> 2) & 3, col & 3
    pick = (((px + block) & 3) << 7) + (((py + step) & 3) << 5) + (pz << 2) + inner
    chosen = (row == pick).astype(f32)
    hidden = jnp.dot(stack[...], chosen, precision=highest, preferred_element_type=f32)
    total = None
    for k, r_ref in enumerate((r0, r1, r2, r3)):
        term = jnp.dot(hidden[:, 16 * k : 16 * k + 16], r_ref[...], precision=highest, preferred_element_type=f32)
        total = term if total is None else total + term
    for k, out_ref in enumerate((o0, o1, o2, o3)):
        out_ref[...] = total[8 * k : 8 * k + 3]


def shifted(array, axis, shift):
    size = lax.axis_size(axis)
    return lax.ppermute(array, axis, [((i + shift) % size, i) for i in range(size)])


def swapped(array):
    return lax.ppermute(array, SHARD, [(0, 1), (1, 0)])


HOPS = ((None, -1), (1, 2), (3, -2), (4, -3))


def hop(array, amounts):
    size = lax.axis_size(Z)
    pairs = []
    for core, by in enumerate(amounts):
        if by is not None:
            pairs += [(i * 2 + core, (i + by) % size * 2 + core) for i in range(size)]
    return lax.ppermute(array, (Z, SHARD), pairs)


def states_along_z(hidden):
    held = [hidden]
    for amounts in ((-1, 1), (-1, 1), (-1, 1), (-1, None)):
        held.append(hop(held[-1], amounts))
    across = lax.ppermute(held[2], SHARD, [(0, 1)])
    return held[1:] + [across]


def first_kernel(place_ref, hidden_hbm, weight_hbm, hidden_ref, weight_ref, info_ref, sems):
    copies = (
        pltpu.make_async_copy(weight_hbm, weight_ref, sems.at[0]),
        pltpu.make_async_copy(hidden_hbm, hidden_ref, sems.at[1]),
    )
    for copy in copies:
        copy.start()
    row = lax.broadcasted_iota(jnp.int32, info_ref.shape, 0)
    info = jnp.zeros(info_ref.shape, jnp.int32)
    for k in range(5):
        info = jnp.where(row == k, place_ref[k], info)
    info_ref[...] = info
    for copy in copies:
        copy.wait()


def brought(place, hidden, weight):
    return call(
        first_kernel, (place, hidden, weight), [IN_SMEM] + [IN_HBM] * 2, vmem((hidden.shape, f32), (weight.shape, f32), ((8, 128), jnp.int32)),
        [IN_VMEM] * 3, [pltpu.SemaphoreType.DMA((2,))], 1, 100_000_000_000,
    )


def line_kernel(r0, r1, r2, r3, out_ref):
    for k, r_ref in enumerate((r0, r1, r2, r3)):
        out_ref[4 * k : 4 * k + 4, :] = r_ref[...]


def sum_kernel(info_ref, own, m0, m1, m2, m3, out_ref):
    out_ref[...] = (jnp.where(info_ref[3:4, 0:1] == 0, own[...], m0[...]) + m1[...]) + (m2[...] + m3[...])


def recurrent_line(weight):
    above = shifted(weight, X, 1)
    below = shifted(weight, X, 3)
    others = (above, shifted(above, X, 1), below)
    shape = (4 * weight.shape[0], weight.shape[1])
    return call(line_kernel, (weight, *others), [IN_VMEM] * 4, vmem((shape, f32)), [IN_VMEM], (), 1, 1 << 16)[0]


def recurrent(hidden, hids, line, info):
    plane = [line]
    for k in (1, 2, 3):
        plane.append(shifted(line, Y, k))
    out = (hidden.shape[0], line.shape[1])
    parts = call(
        recurrent_kernel, (info, hidden, *hids, *plane), [IN_VMEM] * 11,
        vmem(*[(out, f32)] * 4), [IN_VMEM] * 4, [pltpu.VMEM((32, hidden.shape[2]), f32)], 4, 1 << 22,
    )
    moved = [hop(part, HOPS[k]) for k, part in enumerate(parts)]
    return call(
        sum_kernel, (info, parts[0], *moved), [IN_VMEM] * 6,
        vmem((out, f32)), [IN_VMEM], (), 1, 1 << 16,
    )[0]


def update_kernel(
    info_ref,
    mine_ref, theirs_ref, sq_ref, sq_recv_ref, in_w_ref, bias_ref, cell_ref, ctx_w_ref, mlp_ref,
    wg_ref, wu_ref, wd_ref, gg_ref, gu_ref, gd_ref, meta_ref,
    up_g_hbm, up_u_hbm, up_d_hbm, hidden_ref, new_cell_ref, send_ref, keep_ref,
    cell_old, table, table_s, order, sem, sem_out, out_g, out_u, out_d, new_g, new_u, new_d, acc,
):
    count = wg_ref.shape[1] // CHUNK
    units = mlp_ref.shape[1]
    entries = 2.0 * wg_ref.shape[0] * wg_ref.shape[1]

    sums = sq_ref[...] + sq_recv_ref[...]
    total = jnp.sum(sums, axis=1, keepdims=True)
    rms = jnp.sqrt(total / entries + epsilon)
    rms_g, rms_p = rms[0:3], rms[8:11]
    logs = jnp.log(rms)
    fraction = info_ref[4:5, 0:1].astype(f32) / STEPS
    in_w = in_w_ref[...]
    lstm_in = (
        (logs[0:3] * in_w[0:1] + logs[8:11] * in_w[1:2] + fraction * in_w[2:3])
        + (mine_ref[...] + theirs_ref[...])
        + bias_ref[...]
    )
    width = cell_ref.shape[2]
    for j in range(3):
        cell_old[j : j + 1, :] = cell_ref[j]
    in_gate = jax.nn.sigmoid(lstm_in[:, :width])
    forget_gate = jax.nn.sigmoid(lstm_in[:, width : 2 * width])
    candidate = jnp.tanh(lstm_in[:, 2 * width : 3 * width])
    out_gate = jax.nn.sigmoid(lstm_in[:, 3 * width :])
    cell = forget_gate * cell_old[0:3, :] + in_gate * candidate
    hidden = out_gate * jnp.tanh(cell)
    for j in range(3):
        new_cell_ref[j] = cell[j : j + 1]
        hidden_ref[j] = hidden[j : j + 1]
    context = lax.dot_general(
        hidden, ctx_w_ref[...], (((1,), (1,)), ((), ())), precision=highest, preferred_element_type=f32
    )
    mlp = mlp_ref[...]
    out_w = mlp[2:3]
    table[0:3, :units] = out_w * mlp[0:1] / rms_p
    table[8:11, :units] = out_w * mlp[1:2] / rms_g
    table[16:19, :units] = -(out_w * context[:, :units])
    table[24:27, : units + 1] = jnp.exp(context)
    table[32:35, 0:1] = rate_factor * rms_p
    table[40:41, :units] = out_w
    copy = pltpu.make_async_copy(table, table_s, sem)
    copy.start()
    copy.wait()

    positive = jnp.int32(0)
    for k in range(units):
        positive = positive + (table_s[40, k] >= 0).astype(jnp.int32)
    above, below = jnp.int32(0), positive
    for k in range(units):
        is_above = table_s[40, k] >= 0
        spot = jnp.where(is_above, above, below)
        for j in range(3):
            for group in range(3):
                order[group * 12 + j * 4 + spot] = table_s[group * 8 + j, k]
        above = above + is_above.astype(jnp.int32)
        below = below + 1 - is_above.astype(jnp.int32)

    def change(which, j, w_ref, grad_ref, out_ref, new_ref, by_rows, strip):
        scale = table_s[24 + which, units]
        rate = table_s[32 + which, 0]
        a = [order[which * 4 + k] for k in range(units)]
        b = [order[12 + which * 4 + k] for k in range(units)]
        edge = [order[24 + which * 4 + k] for k in range(units)]
        offset = -functools.reduce(lambda s, e: s + e, edge)

        def variant(top):
            def body(i, carry):
                here = pl.ds(pl.multiple_of(i * strip, strip), strip)
                if by_rows:
                    there, lanes = pl.ds(pl.multiple_of(j * CHUNK + i * strip, strip), strip), slice(None)
                else:
                    there, lanes = here, piece(j)
                p = w_ref[there, lanes].astype(f32)
                g = grad_ref[there, lanes]
                total = None
                for k in range(units):
                    term = a[k] * p + b[k] * g
                    term = jnp.maximum(term, edge[k]) if k < top else jnp.minimum(term, edge[k])
                    total = term if total is None else total + term
                upd = scale * (total + offset)
                out_ref[there, lanes] = upd.astype(bf16)
                new_ref[here, :] = (p - rate * upd).astype(bf16)
                return carry

            lax.fori_loop(0, new_ref.shape[0] // strip, body, 0)

        for top in range(units + 1):
            pl.when(positive == top)(functools.partial(variant, top))

    def results(j):
        at = piece(j)
        return (
            pltpu.make_async_copy(out_g.at[:, at], up_g_hbm.at[:, at], sem_out.at[0, j]),
            pltpu.make_async_copy(out_u.at[:, at], up_u_hbm.at[:, at], sem_out.at[1, j]),
            pltpu.make_async_copy(out_d.at[at, :], up_d_hbm.at[at, :], sem_out.at[2, j]),
        )

    def body(j, carry):
        copies = results(j)
        change(0, j, wg_ref, gg_ref, out_g, new_g, False, STRIP)
        copies[0].start()
        change(1, j, wu_ref, gu_ref, out_u, new_u, False, STRIP)
        copies[1].start()
        change(2, j, wd_ref, gd_ref, out_d, new_d, True, STRIP // 4)
        copies[2].start()
        meta = meta_ref[...]
        gate = dot(meta, new_g[...])
        up = dot(meta, new_u[...])
        act = (gate * jax.nn.sigmoid(gate) * up).astype(bf16)
        part = dot(act, new_d[...])

        @pl.when(j == 0)
        def _():
            acc[...] = part

        @pl.when(j > 0)
        def _():
            acc[...] += part

        return carry

    lax.fori_loop(0, count, body, 0)
    half = acc.shape[0] // 2
    lower = info_ref[3:4, 0:1] == 0
    keep_ref[...] = jnp.where(lower, acc[:half], acc[half:])
    send_ref[...] = jnp.where(lower, acc[half:], acc[:half])
    for j in range(count):
        for copy in results(j):
            copy.wait()


STRIP = 64


def update(info, mine, theirs, sums, sums_recv, in_w, bias, cell, ctx_w, mlp, wg, wu, wd, gg, gu, gd, meta):
    tok, width = meta.shape
    hid = wg.shape[1]
    outs = [pltpu.HBM(wg.shape, bf16), pltpu.HBM(wu.shape, bf16), pltpu.HBM(wd.shape, bf16)]
    outs += vmem((cell.shape, f32), (cell.shape, f32), ((tok // 2, width), f32), ((tok // 2, width), f32))
    scratch = [
        pltpu.VMEM((8, cell.shape[2]), f32),
        pltpu.VMEM((48, 128), f32),
        pltpu.SMEM((48, 128), f32),
        pltpu.SMEM((48,), f32),
        pltpu.SemaphoreType.DMA,
        pltpu.SemaphoreType.DMA((3, hid // CHUNK)),
        pltpu.VMEM(wg.shape, bf16),
        pltpu.VMEM(wu.shape, bf16),
        pltpu.VMEM(wd.shape, bf16),
        pltpu.VMEM((width, CHUNK), bf16),
        pltpu.VMEM((width, CHUNK), bf16),
        pltpu.VMEM((CHUNK, width), bf16),
        pltpu.VMEM((tok, width), f32),
    ]
    operands = (info, mine, theirs, sums, sums_recv, in_w, bias, cell, ctx_w, mlp, wg, wu, wd, gg, gu, gd, meta)
    return call(
        update_kernel, operands, [IN_VMEM] * 17,
        outs, [IN_HBM] * 3 + [IN_VMEM] * 4, scratch, 20, 6 * tok * width * hid,
    )


def loss_kernel(scale, info_ref, keep_ref, recv_ref, want_ref, out_ref):
    half = keep_ref.shape[0]
    want = jnp.where(info_ref[3:4, 0:1] == 0, want_ref[:half].astype(f32), want_ref[half:].astype(f32))
    error = keep_ref[...] + recv_ref[...] - want
    total = jnp.sum(jnp.sum(error * error, axis=0, keepdims=True), axis=1, keepdims=True)
    out_ref[...] = jnp.broadcast_to(scale * total, out_ref.shape)


def loss_part(info, keep, recv, want, count):
    scale = 0.5 / (want.shape[0] * want.shape[1]) / count
    return call(
        functools.partial(loss_kernel, scale), (info, keep, recv, want), [IN_VMEM] * 4,
        vmem(((1, 128), f32)), [IN_VMEM], (), 8,
    )[0]


def spread_kernel(mine_ref, theirs_ref, out_ref):
    both = mine_ref[:, 0:1] + theirs_ref[:, 0:1]
    for k in range(out_ref.shape[0]):
        out_ref[k] = both


def spread(part, count):
    return call(spread_kernel, (part, swapped(part)), [IN_VMEM] * 2, vmem(((count, 1, 1), f32)), [IN_VMEM], (), 1)[0]


def local(
    tokens, targets, meta_tokens, meta_targets, gate_weight, up_weight, down_weight, task_step,
    hidden_state, cell_state, recurrent_weight, input_weight, lstm_bias, context_weight, mlp_weight,
):
    core = lax.axis_index(SHARD)
    place = jnp.stack([lax.axis_index(X), lax.axis_index(Y), lax.axis_index(Z), core, task_step[0]]).astype(jnp.int32)
    hidden, weight, info = brought(place, hidden_state.transpose(1, 0, 2), recurrent_weight)
    line = recurrent_line(weight)
    hids = states_along_z(hidden)
    wg, wu, wd = gate_weight[0], up_weight[0], down_weight[0]
    own, p, q, act_t, x_t, param_sq = forward(tokens[0], wg, wu, wd)
    recv = swapped(own)
    mine = recurrent(hidden, hids, line, info)
    gg, gu, gd, sums = backward(own, recv, targets[0], wd, p, q, act_t, x_t, param_sq)
    up_g, up_u, up_d, new_hidden, new_cell, send, keep = update(
        info, mine, swapped(mine), sums, swapped(sums), input_weight, lstm_bias[None], cell_state.transpose(1, 0, 2),
        context_weight.T, mlp_weight, wg, wu, wd, gg, gu, gd, meta_tokens[0],
    )
    count = lax.axis_size(TASK)
    part = loss_part(info, keep, swapped(send), meta_targets[0], count)
    everyone = lax.all_to_all(spread(part, count), TASK, 0, 0, tiled=True)
    meta_loss = jnp.sum(everyone)
    return (
        up_g[None], up_u[None], up_d[None], new_hidden.transpose(1, 0, 2), new_cell.transpose(1, 0, 2), meta_loss
    )


def solution(mesh):
    finer = Mesh(mesh.devices.reshape(4, 4, 8, mesh.shape["shard"]), (X, Y, Z, SHARD))
    return jax.shard_map(
        local,
        mesh=finer,
        in_specs=(
            P(TASK, None, None), P(TASK, None, None), P(TASK, None, None), P(TASK, None, None),
            P(TASK, None, "shard"), P(TASK, None, "shard"), P(TASK, "shard", None), P(TASK),
            P(TASK, None, None), P(TASK, None, None), P(TASK, None), P(), P(), P(), P(),
        ),
        out_specs=(
            P(TASK, None, "shard"), P(TASK, None, "shard"), P(TASK, "shard", None),
            P(TASK, None, None), P(TASK, None, None), P(),
        ),
        check_vma=False,
    )
```

```python
import functools

import jax
import jax.numpy as jnp
from jax import lax
from jax.experimental import pallas as pl
from jax.experimental.pallas import tpu as pltpu
from jax.sharding import Mesh
from jax.sharding import PartitionSpec as P


STEPS = 10000
X, Y, Z, SHARD = "task_0", "task_1", "task_2", "shard"
TASK = (X, Y, Z)

f32, bf16 = jnp.float32, jnp.bfloat16
highest = lax.Precision.HIGHEST
epsilon = 1e-06
rate_factor = 0.1
CHUNK = 256
MIB = 1 << 20


def dot(a, b):
    return jnp.dot(a, b, preferred_element_type=f32)


def dot_t(a, b):
    return lax.dot_general(a, b, (((1,), (1,)), ((), ())), preferred_element_type=f32)


def lane_sums(value):
    sums = jnp.sum(value, axis=0, keepdims=True)
    total = sums[:, :128]
    for start in range(128, sums.shape[1], 128):
        total = total + sums[:, start : start + 128]
    return total


def squares(value):
    value = value.astype(f32)
    return lane_sums(value * value)


def vmem(*shapes):
    return [pltpu.VMEM(shape, kind) for shape, kind in shapes]


IN_VMEM = pl.BlockSpec(memory_space=pltpu.VMEM)
IN_HBM = pl.BlockSpec(memory_space=pltpu.HBM)
IN_SMEM = pl.BlockSpec(memory_space=pltpu.SMEM)


def call(body, operands, specs, outs, out_specs, scratch=(), limit=8, flops=0):
    held = [pltpu.with_memory_space_constraint(a, pltpu.HBM) if spec is IN_HBM else a for a, spec in zip(operands, specs)]
    return pl.pallas_call(
        body,
        in_specs=specs,
        out_specs=out_specs,
        out_shape=outs,
        scratch_shapes=scratch,
        compiler_params=pltpu.CompilerParams(vmem_limit_bytes=limit * MIB),
        cost_estimate=pl.CostEstimate(flops=flops, transcendentals=0, bytes_accessed=0) if flops else None,
    )(*held)


def piece(j):
    return pl.ds(pl.multiple_of(j * CHUNK, CHUNK), CHUNK)


def forward_kernel(x_ref, wg_ref, wu_ref, wd_ref, out_ref, p_ref, q_ref, act_t_ref, x_t_ref, sq_ref):
    sq_ref[...] = jnp.zeros_like(sq_ref)

    def body(j, carry):
        at = piece(j)
        x = x_ref[...]
        gate = dot(x, wg_ref[:, at])
        up = dot(x, wu_ref[:, at])
        sig = jax.nn.sigmoid(gate)
        silu = gate * sig
        q_ref[:, at] = silu
        p_ref[:, at] = up * sig * (1.0 + gate * (1.0 - sig))
        act = (silu * up).astype(bf16)
        act_t_ref[at, :] = act.T
        part = dot(act, wd_ref[at, :])

        @pl.when(j == 0)
        def _():
            out_ref[...] = part
            x_t_ref[...] = x_ref[...].T

        @pl.when(j > 0)
        def _():
            out_ref[...] += part

        sq_ref[0:1, :] += squares(wg_ref[:, at])
        sq_ref[1:2, :] += squares(wu_ref[:, at])
        sq_ref[2:3, :] += squares(wd_ref[at, :])
        return carry

    lax.fori_loop(0, wg_ref.shape[1] // CHUNK, body, 0)


def forward(x, wg, wu, wd):
    tok, width = x.shape
    hid = wg.shape[1]
    outs = vmem(
        ((tok, width), f32), ((tok, hid), f32), ((tok, hid), f32), ((hid, tok), bf16), ((width, tok), bf16), ((8, 128), f32),
    )
    return call(
        forward_kernel, (x, wg, wu, wd), [IN_VMEM] * 4,
        outs, [IN_VMEM] * len(outs), (), 8, 6 * tok * width * hid,
    )


def backward_kernel(
    own_ref, recv_ref, want_ref, wd_ref, p_ref, q_ref, act_t_ref, x_t_ref, psq_ref, gg_ref, gu_ref, gd_ref, sq_ref, d_out_ref
):
    sq_ref[0:8, :] = jnp.zeros_like(psq_ref)
    sq_ref[8:16, :] = psq_ref[...]
    d_out_ref[...] = (own_ref[...] + recv_ref[...] - want_ref[...].astype(f32)).astype(bf16)

    def body(j, carry):
        at = piece(j)
        d_out = d_out_ref[...]
        d_act = dot_t(d_out, wd_ref[at, :])
        dg = (d_act * p_ref[:, at]).astype(bf16)
        du = (d_act * q_ref[:, at]).astype(bf16)
        x_t = x_t_ref[...]
        grad = dot(x_t, dg)
        gg_ref[:, at] = grad
        sq_ref[0:1, :] += squares(grad)
        grad = dot(x_t, du)
        gu_ref[:, at] = grad
        sq_ref[1:2, :] += squares(grad)
        grad = dot(act_t_ref[at, :], d_out)
        gd_ref[at, :] = grad
        sq_ref[2:3, :] += squares(grad)
        return carry

    lax.fori_loop(0, wd_ref.shape[0] // CHUNK, body, 0)


def backward(own, recv, want, wd, p, q, act_t, x_t, param_sq):
    tok, width = own.shape
    hid = wd.shape[0]
    outs = vmem(((width, hid), f32), ((width, hid), f32), ((hid, width), f32), ((16, 128), f32))
    return call(
        backward_kernel, (own, recv, want, wd, p, q, act_t, x_t, param_sq), [IN_VMEM] * 9,
        outs, [IN_VMEM] * 4, [pltpu.VMEM((tok, width), bf16)], 12, 8 * tok * width * hid,
    )


def recurrent_kernel(info_ref, h0, h1, h2, h3, r0, r1, r2, r3, o0, o1, o2, o3, stack):
    px, py, pz, core = (info_ref[k : k + 1, 0:1] for k in range(4))
    state = h0.shape[2]
    stack[...] = jnp.zeros_like(stack)
    for k, hid_ref in enumerate((h0, h1, h2, h3)):
        for j in range(hid_ref.shape[0]):
            stack[8 * k + j : 8 * k + j + 1, :] = hid_ref[j]
    shape = (state, 128)
    row = lax.broadcasted_iota(jnp.int32, shape, 0)
    col = lax.broadcasted_iota(jnp.int32, (1, 128), 1)
    step, block, inner = col >> 4, (col >> 2) & 3, col & 3
    away = jnp.zeros((1, 128), jnp.int32)
    for k, (south, north) in enumerate(HOPS):
        away = jnp.where(block == k, jnp.where(core == 0, south, north), away)
    pick = (px << 7) + (((py + step) & 3) << 5) + (((pz + away) & 7) << 2) + inner
    chosen = (row == pick).astype(f32)
    hidden = jnp.dot(stack[...], chosen, precision=highest, preferred_element_type=f32)
    total = None
    for k, r_ref in enumerate((r0, r1, r2, r3)):
        term = jnp.dot(hidden[:, 16 * k : 16 * k + 16], r_ref[...], precision=highest, preferred_element_type=f32)
        total = term if total is None else total + term
    for k, out_ref in enumerate((o0, o1, o2, o3)):
        out_ref[...] = total[8 * k : 8 * k + 3]


def shifted(array, axis, shift):
    size = lax.axis_size(axis)
    return lax.ppermute(array, axis, [((i + shift) % size, i) for i in range(size)])


def swapped(array):
    return lax.ppermute(array, SHARD, [(0, 1), (1, 0)])


HOPS = ((0, 1), (2, -1), (3, -2), (4, -3))


def from_along_z(array, amounts):
    size = lax.axis_size(Z)
    pairs = []
    for core, by in enumerate(amounts):
        if by != 0:
            pairs += [((i + by) % size * 2 + core, i * 2 + core) for i in range(size)]
    return lax.ppermute(array, (Z, SHARD), pairs)


def first_kernel(place_ref, hidden_hbm, weight_hbm, hidden_ref, weight_ref, info_ref, sems):
    copies = (
        pltpu.make_async_copy(weight_hbm, weight_ref, sems.at[0]),
        pltpu.make_async_copy(hidden_hbm, hidden_ref, sems.at[1]),
    )
    for copy in copies:
        copy.start()
    row = lax.broadcasted_iota(jnp.int32, info_ref.shape, 0)
    info = jnp.zeros(info_ref.shape, jnp.int32)
    for k in range(5):
        info = jnp.where(row == k, place_ref[k], info)
    info_ref[...] = info
    for copy in copies:
        copy.wait()


def brought(place, hidden, weight):
    return call(
        first_kernel, (place, hidden, weight), [IN_SMEM] + [IN_HBM] * 2,
        vmem((hidden.shape, f32), (weight.shape, f32), ((8, 128), jnp.int32)),
        [IN_VMEM] * 3, [pltpu.SemaphoreType.DMA((2,))], 1, 100_000_000_000,
    )


def line_kernel(info_ref, own, r0, r1, r2, r3, out_ref):
    out_ref[0:4, :] = jnp.where(info_ref[3:4, 0:1] == 0, own[...], r0[...])
    for k, r_ref in enumerate((r1, r2, r3)):
        out_ref[4 * k + 4 : 4 * k + 8, :] = r_ref[...]


def sum_kernel(own, m1, m2, m3, out_ref):
    out_ref[...] = (own[...] + m1[...]) + (m2[...] + m3[...])


def recurrent_line(weight, info):
    others = [from_along_z(weight, amounts) for amounts in HOPS]
    shape = (4 * weight.shape[0], weight.shape[1])
    return call(line_kernel, (info, weight, *others), [IN_VMEM] * 6, vmem((shape, f32)), [IN_VMEM], (), 1, 1 << 16)[0]


def recurrent(hids, line, info):
    plane = [line] + [shifted(line, Y, k) for k in (1, 2, 3)]
    out = (hids[0].shape[0], line.shape[1])
    parts = call(
        recurrent_kernel, (info, *hids, *plane), [IN_VMEM] * 9,
        vmem(*[(out, f32)] * 4), [IN_VMEM] * 4, [pltpu.VMEM((32, hids[0].shape[2]), f32)], 4, 1 << 22,
    )
    moved = [shifted(parts[k], X, -k) for k in (1, 2, 3)]
    return call(sum_kernel, (parts[0], *moved), [IN_VMEM] * 4, vmem((out, f32)), [IN_VMEM], (), 1, 1 << 16)[0]


def update_kernel(
    info_ref,
    mine_ref, theirs_ref, sq_ref, sq_recv_ref, in_w_ref, bias_ref, cell_ref, ctx_w_ref, mlp_ref,
    wg_ref, wu_ref, wd_ref, gg_ref, gu_ref, gd_ref, meta_ref,
    up_g_hbm, up_u_hbm, up_d_hbm, hidden_ref, new_cell_ref, send_ref, keep_ref,
    cell_old, table, table_s, order, sem, sem_out, out_g, out_u, out_d, new_g, new_u, new_d, acc,
):
    count = wg_ref.shape[1] // CHUNK
    units = mlp_ref.shape[1]
    entries = 2.0 * wg_ref.shape[0] * wg_ref.shape[1]

    sums = sq_ref[...] + sq_recv_ref[...]
    total = jnp.sum(sums, axis=1, keepdims=True)
    rms = jnp.sqrt(total / entries + epsilon)
    rms_g, rms_p = rms[0:3], rms[8:11]
    logs = jnp.log(rms)
    fraction = info_ref[4:5, 0:1].astype(f32) / STEPS
    in_w = in_w_ref[...]
    lstm_in = (
        (logs[0:3] * in_w[0:1] + logs[8:11] * in_w[1:2] + fraction * in_w[2:3])
        + (mine_ref[...] + theirs_ref[...])
        + bias_ref[...]
    )
    width = cell_ref.shape[2]
    for j in range(3):
        cell_old[j : j + 1, :] = cell_ref[j]
    in_gate = jax.nn.sigmoid(lstm_in[:, :width])
    forget_gate = jax.nn.sigmoid(lstm_in[:, width : 2 * width])
    candidate = jnp.tanh(lstm_in[:, 2 * width : 3 * width])
    out_gate = jax.nn.sigmoid(lstm_in[:, 3 * width :])
    cell = forget_gate * cell_old[0:3, :] + in_gate * candidate
    hidden = out_gate * jnp.tanh(cell)
    for j in range(3):
        new_cell_ref[j] = cell[j : j + 1]
        hidden_ref[j] = hidden[j : j + 1]
    context = lax.dot_general(
        hidden, ctx_w_ref[...], (((1,), (1,)), ((), ())), precision=highest, preferred_element_type=f32
    )
    mlp = mlp_ref[...]
    out_w = mlp[2:3]
    table[0:3, :units] = out_w * mlp[0:1] / rms_p
    table[8:11, :units] = out_w * mlp[1:2] / rms_g
    table[16:19, :units] = -(out_w * context[:, :units])
    table[24:27, : units + 1] = jnp.exp(context)
    table[32:35, 0:1] = rate_factor * rms_p
    table[40:41, :units] = out_w
    copy = pltpu.make_async_copy(table, table_s, sem)
    copy.start()
    copy.wait()

    positive = jnp.int32(0)
    for k in range(units):
        positive = positive + (table_s[40, k] >= 0).astype(jnp.int32)
    above, below = jnp.int32(0), positive
    for k in range(units):
        is_above = table_s[40, k] >= 0
        spot = jnp.where(is_above, above, below)
        for j in range(3):
            for group in range(3):
                order[group * 12 + j * 4 + spot] = table_s[group * 8 + j, k]
        above = above + is_above.astype(jnp.int32)
        below = below + 1 - is_above.astype(jnp.int32)

    def change(which, j, w_ref, grad_ref, out_ref, new_ref, by_rows, strip):
        scale = table_s[24 + which, units]
        rate = table_s[32 + which, 0]
        a = [order[which * 4 + k] for k in range(units)]
        b = [order[12 + which * 4 + k] for k in range(units)]
        edge = [order[24 + which * 4 + k] for k in range(units)]
        offset = -functools.reduce(lambda s, e: s + e, edge)

        def variant(top):
            def body(i, carry):
                here = pl.ds(pl.multiple_of(i * strip, strip), strip)
                if by_rows:
                    there, lanes = pl.ds(pl.multiple_of(j * CHUNK + i * strip, strip), strip), slice(None)
                else:
                    there, lanes = here, piece(j)
                p = w_ref[there, lanes].astype(f32)
                g = grad_ref[there, lanes]
                total = None
                for k in range(units):
                    term = a[k] * p + b[k] * g
                    term = jnp.maximum(term, edge[k]) if k < top else jnp.minimum(term, edge[k])
                    total = term if total is None else total + term
                upd = scale * (total + offset)
                out_ref[there, lanes] = upd.astype(bf16)
                new_ref[here, :] = (p - rate * upd).astype(bf16)
                return carry

            lax.fori_loop(0, new_ref.shape[0] // strip, body, 0)

        for top in range(units + 1):
            pl.when(positive == top)(functools.partial(variant, top))

    def results(j):
        at = piece(j)
        return (
            pltpu.make_async_copy(out_g.at[:, at], up_g_hbm.at[:, at], sem_out.at[0, j]),
            pltpu.make_async_copy(out_u.at[:, at], up_u_hbm.at[:, at], sem_out.at[1, j]),
            pltpu.make_async_copy(out_d.at[at, :], up_d_hbm.at[at, :], sem_out.at[2, j]),
        )

    def body(j, carry):
        copies = results(j)
        change(0, j, wg_ref, gg_ref, out_g, new_g, False, STRIP)
        copies[0].start()
        change(1, j, wu_ref, gu_ref, out_u, new_u, False, STRIP)
        copies[1].start()
        change(2, j, wd_ref, gd_ref, out_d, new_d, True, STRIP // 4)
        copies[2].start()
        meta = meta_ref[...]
        gate = dot(meta, new_g[...])
        up = dot(meta, new_u[...])
        act = (gate * jax.nn.sigmoid(gate) * up).astype(bf16)
        part = dot(act, new_d[...])

        @pl.when(j == 0)
        def _():
            acc[...] = part

        @pl.when(j > 0)
        def _():
            acc[...] += part

        return carry

    lax.fori_loop(0, count, body, 0)
    half = acc.shape[0] // 2
    lower = info_ref[3:4, 0:1] == 0
    keep_ref[...] = jnp.where(lower, acc[:half], acc[half:])
    send_ref[...] = jnp.where(lower, acc[half:], acc[:half])
    for j in range(count):
        for copy in results(j):
            copy.wait()


STRIP = 64


def update(info, mine, theirs, sums, sums_recv, in_w, bias, cell, ctx_w, mlp, wg, wu, wd, gg, gu, gd, meta):
    tok, width = meta.shape
    hid = wg.shape[1]
    outs = [pltpu.HBM(wg.shape, bf16), pltpu.HBM(wu.shape, bf16), pltpu.HBM(wd.shape, bf16)]
    outs += vmem((cell.shape, f32), (cell.shape, f32), ((tok // 2, width), f32), ((tok // 2, width), f32))
    scratch = [
        pltpu.VMEM((8, cell.shape[2]), f32),
        pltpu.VMEM((48, 128), f32),
        pltpu.SMEM((48, 128), f32),
        pltpu.SMEM((48,), f32),
        pltpu.SemaphoreType.DMA,
        pltpu.SemaphoreType.DMA((3, hid // CHUNK)),
        pltpu.VMEM(wg.shape, bf16),
        pltpu.VMEM(wu.shape, bf16),
        pltpu.VMEM(wd.shape, bf16),
        pltpu.VMEM((width, CHUNK), bf16),
        pltpu.VMEM((width, CHUNK), bf16),
        pltpu.VMEM((CHUNK, width), bf16),
        pltpu.VMEM((tok, width), f32),
    ]
    operands = (info, mine, theirs, sums, sums_recv, in_w, bias, cell, ctx_w, mlp, wg, wu, wd, gg, gu, gd, meta)
    return call(
        update_kernel, operands, [IN_VMEM] * 17,
        outs, [IN_HBM] * 3 + [IN_VMEM] * 4, scratch, 20, 6 * tok * width * hid,
    )


def loss_kernel(scale, info_ref, keep_ref, recv_ref, want_ref, out_ref):
    half = keep_ref.shape[0]
    want = jnp.where(info_ref[3:4, 0:1] == 0, want_ref[:half].astype(f32), want_ref[half:].astype(f32))
    error = keep_ref[...] + recv_ref[...] - want
    total = jnp.sum(jnp.sum(error * error, axis=0, keepdims=True), axis=1, keepdims=True)
    out_ref[...] = jnp.broadcast_to(scale * total, out_ref.shape)


def loss_part(info, keep, recv, want, count):
    scale = 0.5 / (want.shape[0] * want.shape[1]) / count
    return call(
        functools.partial(loss_kernel, scale), (info, keep, recv, want), [IN_VMEM] * 4,
        vmem(((1, 128), f32)), [IN_VMEM], (), 8,
    )[0]


def spread_kernel(mine_ref, theirs_ref, out_ref):
    both = mine_ref[:, 0:1] + theirs_ref[:, 0:1]
    for k in range(out_ref.shape[0]):
        out_ref[k] = both


def spread(part, count):
    return call(spread_kernel, (part, swapped(part)), [IN_VMEM] * 2, vmem(((count, 1, 1), f32)), [IN_VMEM], (), 1)[0]


def local(
    tokens, targets, meta_tokens, meta_targets, gate_weight, up_weight, down_weight, task_step,
    hidden_state, cell_state, recurrent_weight, input_weight, lstm_bias, context_weight, mlp_weight,
):
    core = lax.axis_index(SHARD)
    place = jnp.stack([lax.axis_index(X), lax.axis_index(Y), lax.axis_index(Z), core, task_step[0]]).astype(jnp.int32)
    hidden, weight, info = brought(place, hidden_state.transpose(1, 0, 2), recurrent_weight)
    line = recurrent_line(weight, info)
    hids = [hidden] + [shifted(hidden, X, k) for k in (1, 2, 3)]
    wg, wu, wd = gate_weight[0], up_weight[0], down_weight[0]
    own, p, q, act_t, x_t, param_sq = forward(tokens[0], wg, wu, wd)
    recv = swapped(own)
    mine = recurrent(hids, line, info)
    gg, gu, gd, sums = backward(own, recv, targets[0], wd, p, q, act_t, x_t, param_sq)
    up_g, up_u, up_d, new_hidden, new_cell, send, keep = update(
        info, mine, swapped(mine), sums, swapped(sums), input_weight, lstm_bias[None], cell_state.transpose(1, 0, 2),
        context_weight.T, mlp_weight, wg, wu, wd, gg, gu, gd, meta_tokens[0],
    )
    count = lax.axis_size(TASK)
    part = loss_part(info, keep, swapped(send), meta_targets[0], count)
    everyone = lax.all_to_all(spread(part, count), TASK, 0, 0, tiled=True)
    meta_loss = jnp.sum(everyone)
    return (
        up_g[None], up_u[None], up_d[None], new_hidden.transpose(1, 0, 2), new_cell.transpose(1, 0, 2), meta_loss
    )


def solution(mesh):
    finer = Mesh(mesh.devices.reshape(4, 4, 8, mesh.shape["shard"]), (X, Y, Z, SHARD))
    return jax.shard_map(
        local,
        mesh=finer,
        in_specs=(
            P(TASK, None, None), P(TASK, None, None), P(TASK, None, None), P(TASK, None, None),
            P(TASK, None, "shard"), P(TASK, None, "shard"), P(TASK, "shard", None), P(TASK),
            P(TASK, None, None), P(TASK, None, None), P(TASK, None), P(), P(), P(), P(),
        ),
        out_specs=(
            P(TASK, None, "shard"), P(TASK, None, "shard"), P(TASK, "shard", None),
            P(TASK, None, None), P(TASK, None, None), P(),
        ),
        check_vma=False,
    )
```

```python
import functools

import jax
import jax.numpy as jnp
from jax import lax
from jax.experimental import pallas as pl
from jax.experimental.pallas import tpu as pltpu
from jax.sharding import Mesh
from jax.sharding import PartitionSpec as P


STEPS = 10000
X, Y, Z, SHARD = "task_0", "task_1", "task_2", "shard"
TASK = (X, Y, Z)

f32, bf16 = jnp.float32, jnp.bfloat16
highest = lax.Precision.HIGHEST
epsilon = 1e-06
rate_factor = 0.1
CHUNK = 256
MIB = 1 << 20


def dot(a, b):
    return jnp.dot(a, b, preferred_element_type=f32)


def dot_t(a, b):
    return lax.dot_general(a, b, (((1,), (1,)), ((), ())), preferred_element_type=f32)


def lane_sums(value):
    sums = jnp.sum(value, axis=0, keepdims=True)
    total = sums[:, :128]
    for start in range(128, sums.shape[1], 128):
        total = total + sums[:, start : start + 128]
    return total


def squares(value):
    value = value.astype(f32)
    return lane_sums(value * value)


def vmem(*shapes):
    return [pltpu.VMEM(shape, kind) for shape, kind in shapes]


IN_VMEM = pl.BlockSpec(memory_space=pltpu.VMEM)
IN_HBM = pl.BlockSpec(memory_space=pltpu.HBM)
IN_SMEM = pl.BlockSpec(memory_space=pltpu.SMEM)


def call(body, operands, specs, outs, out_specs, scratch=(), limit=8, flops=0):
    held = [pltpu.with_memory_space_constraint(a, pltpu.HBM) if spec is IN_HBM else a for a, spec in zip(operands, specs)]
    return pl.pallas_call(
        body,
        in_specs=specs,
        out_specs=out_specs,
        out_shape=outs,
        scratch_shapes=scratch,
        compiler_params=pltpu.CompilerParams(vmem_limit_bytes=limit * MIB),
        cost_estimate=pl.CostEstimate(flops=flops, transcendentals=0, bytes_accessed=0) if flops else None,
    )(*held)


def piece(j):
    return pl.ds(pl.multiple_of(j * CHUNK, CHUNK), CHUNK)


def forward_kernel(x_ref, wg_ref, wu_ref, wd_ref, out_ref, p_ref, q_ref, act_t_ref, x_t_ref, sq_ref):
    sq_ref[...] = jnp.zeros_like(sq_ref)

    def body(j, carry):
        at = piece(j)
        x = x_ref[...]
        gate = dot(x, wg_ref[:, at])
        up = dot(x, wu_ref[:, at])
        sig = jax.nn.sigmoid(gate)
        silu = gate * sig
        q_ref[:, at] = silu
        p_ref[:, at] = up * sig * (1.0 + gate * (1.0 - sig))
        act = (silu * up).astype(bf16)
        act_t_ref[at, :] = act.T
        part = dot(act, wd_ref[at, :])

        @pl.when(j == 0)
        def _():
            out_ref[...] = part
            x_t_ref[...] = x_ref[...].T

        @pl.when(j > 0)
        def _():
            out_ref[...] += part

        sq_ref[0:1, :] += squares(wg_ref[:, at])
        sq_ref[1:2, :] += squares(wu_ref[:, at])
        sq_ref[2:3, :] += squares(wd_ref[at, :])
        return carry

    lax.fori_loop(0, wg_ref.shape[1] // CHUNK, body, 0)


def forward(x, wg, wu, wd):
    tok, width = x.shape
    hid = wg.shape[1]
    outs = vmem(
        ((tok, width), f32), ((tok, hid), f32), ((tok, hid), f32), ((hid, tok), bf16), ((width, tok), bf16), ((8, 128), f32),
    )
    return call(
        forward_kernel, (x, wg, wu, wd), [IN_VMEM] * 4,
        outs, [IN_VMEM] * len(outs), (), 8, 6 * tok * width * hid,
    )


def backward_kernel(
    own_ref, recv_ref, want_ref, wd_ref, p_ref, q_ref, act_t_ref, x_t_ref, psq_ref, gg_ref, gu_ref, gd_ref, sq_ref, d_out_ref
):
    sq_ref[0:8, :] = jnp.zeros_like(psq_ref)
    sq_ref[8:16, :] = psq_ref[...]
    d_out_ref[...] = (own_ref[...] + recv_ref[...] - want_ref[...].astype(f32)).astype(bf16)

    def body(j, carry):
        at = piece(j)
        d_out = d_out_ref[...]
        d_act = dot_t(d_out, wd_ref[at, :])
        dg = (d_act * p_ref[:, at]).astype(bf16)
        du = (d_act * q_ref[:, at]).astype(bf16)
        x_t = x_t_ref[...]
        grad = dot(x_t, dg)
        gg_ref[:, at] = grad
        sq_ref[0:1, :] += squares(grad)
        grad = dot(x_t, du)
        gu_ref[:, at] = grad
        sq_ref[1:2, :] += squares(grad)
        grad = dot(act_t_ref[at, :], d_out)
        gd_ref[at, :] = grad
        sq_ref[2:3, :] += squares(grad)
        return carry

    lax.fori_loop(0, wd_ref.shape[0] // CHUNK, body, 0)


def backward(own, recv, want, wd, p, q, act_t, x_t, param_sq):
    tok, width = own.shape
    hid = wd.shape[0]
    outs = vmem(((width, hid), f32), ((width, hid), f32), ((hid, width), f32), ((16, 128), f32))
    return call(
        backward_kernel, (own, recv, want, wd, p, q, act_t, x_t, param_sq), [IN_VMEM] * 9,
        outs, [IN_VMEM] * 4, [pltpu.VMEM((tok, width), bf16)], 12, 8 * tok * width * hid,
    )


def recurrent_kernel(info_ref, h0, h1, h2, h3, r0, r1, r2, r3, o0, o1, o2, o3, stack):
    px, py, pz, core = (info_ref[k : k + 1, 0:1] for k in range(4))
    state = h0.shape[2]
    stack[...] = jnp.zeros_like(stack)
    for k, hid_ref in enumerate((h0, h1, h2, h3)):
        for j in range(hid_ref.shape[0]):
            stack[8 * k + j : 8 * k + j + 1, :] = hid_ref[j]
    shape = (state, 128)
    row = lax.broadcasted_iota(jnp.int32, shape, 0)
    col = lax.broadcasted_iota(jnp.int32, (1, 128), 1)
    step, block, inner = col >> 4, (col >> 2) & 3, col & 3
    away = jnp.zeros((1, 128), jnp.int32)
    for k, (south, north) in enumerate(HOPS):
        away = jnp.where(block == k, jnp.where(core == 0, south, north), away)
    pick = (px << 7) + (((py + step) & 3) << 5) + (((pz + away) & 7) << 2) + inner
    chosen = (row == pick).astype(f32)
    hidden = jnp.dot(stack[...], chosen, precision=highest, preferred_element_type=f32)
    total = None
    for k, r_ref in enumerate((r0, r1, r2, r3)):
        term = jnp.dot(hidden[:, 16 * k : 16 * k + 16], r_ref[...], precision=highest, preferred_element_type=f32)
        total = term if total is None else total + term
    for k, out_ref in enumerate((o0, o1, o2, o3)):
        out_ref[...] = total[8 * k : 8 * k + 3]


def shifted(array, axis, shift):
    size = lax.axis_size(axis)
    return lax.ppermute(array, axis, [((i + shift) % size, i) for i in range(size)])


def swapped(array):
    return lax.ppermute(array, SHARD, [(0, 1), (1, 0)])


HOPS = ((0, 1), (2, -1), (3, -2), (4, -3))


def from_along_z(array, amounts):
    size = lax.axis_size(Z)
    pairs = []
    for core, by in enumerate(amounts):
        if by != 0:
            pairs += [((i + by) % size * 2 + core, i * 2 + core) for i in range(size)]
    return lax.ppermute(array, (Z, SHARD), pairs)


def first_kernel(place_ref, hidden_hbm, weight_hbm, hidden_ref, weight_ref, info_ref, sems):
    copies = (
        pltpu.make_async_copy(weight_hbm, weight_ref, sems.at[0]),
        pltpu.make_async_copy(hidden_hbm, hidden_ref, sems.at[1]),
    )
    for copy in copies:
        copy.start()
    row = lax.broadcasted_iota(jnp.int32, info_ref.shape, 0)
    info = jnp.zeros(info_ref.shape, jnp.int32)
    for k in range(5):
        info = jnp.where(row == k, place_ref[k], info)
    info_ref[...] = info
    for copy in copies:
        copy.wait()


def brought(place, hidden, weight):
    return call(
        first_kernel, (place, hidden, weight), [IN_SMEM] + [IN_HBM] * 2,
        vmem((hidden.shape, f32), (weight.shape, f32), ((8, 128), jnp.int32)),
        [IN_VMEM] * 3, [pltpu.SemaphoreType.DMA((2,))], 1, 100_000_000_000,
    )


def line_kernel(info_ref, own, r0, r1, r2, r3, out_ref):
    out_ref[0:4, :] = jnp.where(info_ref[3:4, 0:1] == 0, own[...], r0[...])
    for k, r_ref in enumerate((r1, r2, r3)):
        out_ref[4 * k + 4 : 4 * k + 8, :] = r_ref[...]


def sum_kernel(own, m1, m2, m3, out_ref):
    out_ref[...] = (own[...] + m1[...]) + (m2[...] + m3[...])


def recurrent_line(held, weight, info):
    others = [from_along_z(held, amounts) for amounts in HOPS]
    shape = (4 * weight.shape[0], weight.shape[1])
    return call(line_kernel, (info, weight, *others), [IN_VMEM] * 6, vmem((shape, f32)), [IN_VMEM], (), 1, 1 << 16)[0]


def recurrent(hids, line, info):
    plane = [line] + [shifted(line, Y, k) for k in (1, 2, 3)]
    out = (hids[0].shape[0], line.shape[1])
    parts = call(
        recurrent_kernel, (info, *hids, *plane), [IN_VMEM] * 9,
        vmem(*[(out, f32)] * 4), [IN_VMEM] * 4, [pltpu.VMEM((32, hids[0].shape[2]), f32)], 4, 1 << 22,
    )
    moved = [shifted(parts[k], X, -k) for k in (1, 2, 3)]
    return call(sum_kernel, (parts[0], *moved), [IN_VMEM] * 4, vmem((out, f32)), [IN_VMEM], (), 1, 1 << 16)[0]


def meta_piece(j, meta, new_g, new_u, new_d, acc):
    at = piece(j)
    gate = dot(meta, new_g[:, at])
    up = dot(meta, new_u[:, at])
    act = (gate * jax.nn.sigmoid(gate) * up).astype(bf16)
    part = dot(act, new_d[at, :])

    @pl.when(j == 0)
    def _():
        acc[...] = part

    @pl.when(j > 0)
    def _():
        acc[...] += part


def keep_kernel(info_ref, meta_ref, new_g, new_u, new_d, keep_ref, mine):
    half = mine.shape[0]
    mine[...] = jnp.where(info_ref[3:4, 0:1] == 0, meta_ref[:half], meta_ref[half:])

    def body(j, carry):
        meta_piece(j, mine[...], new_g, new_u, new_d, keep_ref)
        return carry

    lax.fori_loop(0, new_d.shape[0] // CHUNK, body, 0)


def kept(info, meta, new_g, new_u, new_d):
    tok, width = meta.shape
    return call(
        keep_kernel, (info, meta, new_g, new_u, new_d), [IN_VMEM] * 5,
        vmem(((tok // 2, width), f32)), [IN_VMEM], [pltpu.VMEM((tok // 2, width), bf16)], 6, 1 << 30,
    )[0]


def update_kernel(
    info_ref,
    mine_ref, theirs_ref, sq_ref, sq_recv_ref, in_w_ref, bias_ref, cell_ref, ctx_w_ref, mlp_ref,
    wg_ref, wu_ref, wd_ref, gg_ref, gu_ref, gd_ref, meta_ref,
    up_g_hbm, up_u_hbm, up_d_hbm, hidden_ref, new_cell_ref, send_ref, new_g, new_u, new_d,
    cell_old, table, table_s, order, sem, sem_out, out_g, out_u, out_d, theirs,
):
    count = wg_ref.shape[1] // CHUNK
    units = mlp_ref.shape[1]
    entries = 2.0 * wg_ref.shape[0] * wg_ref.shape[1]

    sums = sq_ref[...] + sq_recv_ref[...]
    total = jnp.sum(sums, axis=1, keepdims=True)
    rms = jnp.sqrt(total / entries + epsilon)
    rms_g, rms_p = rms[0:3], rms[8:11]
    logs = jnp.log(rms)
    fraction = info_ref[4:5, 0:1].astype(f32) / STEPS
    in_w = in_w_ref[...]
    lstm_in = (
        (logs[0:3] * in_w[0:1] + logs[8:11] * in_w[1:2] + fraction * in_w[2:3])
        + (mine_ref[...] + theirs_ref[...])
        + bias_ref[...]
    )
    width = cell_ref.shape[2]
    for j in range(3):
        cell_old[j : j + 1, :] = cell_ref[j]
    in_gate = jax.nn.sigmoid(lstm_in[:, :width])
    forget_gate = jax.nn.sigmoid(lstm_in[:, width : 2 * width])
    candidate = jnp.tanh(lstm_in[:, 2 * width : 3 * width])
    out_gate = jax.nn.sigmoid(lstm_in[:, 3 * width :])
    cell = forget_gate * cell_old[0:3, :] + in_gate * candidate
    hidden = out_gate * jnp.tanh(cell)
    for j in range(3):
        new_cell_ref[j] = cell[j : j + 1]
        hidden_ref[j] = hidden[j : j + 1]
    context = lax.dot_general(
        hidden, ctx_w_ref[...], (((1,), (1,)), ((), ())), precision=highest, preferred_element_type=f32
    )
    mlp = mlp_ref[...]
    out_w = mlp[2:3]
    table[0:3, :units] = out_w * mlp[0:1] / rms_p
    table[8:11, :units] = out_w * mlp[1:2] / rms_g
    table[16:19, :units] = -(out_w * context[:, :units])
    table[24:27, : units + 1] = jnp.exp(context)
    table[32:35, 0:1] = rate_factor * rms_p
    table[40:41, :units] = out_w
    copy = pltpu.make_async_copy(table, table_s, sem)
    copy.start()
    copy.wait()

    positive = jnp.int32(0)
    for k in range(units):
        positive = positive + (table_s[40, k] >= 0).astype(jnp.int32)
    above, below = jnp.int32(0), positive
    for k in range(units):
        is_above = table_s[40, k] >= 0
        spot = jnp.where(is_above, above, below)
        for j in range(3):
            for group in range(3):
                order[group * 12 + j * 4 + spot] = table_s[group * 8 + j, k]
        above = above + is_above.astype(jnp.int32)
        below = below + 1 - is_above.astype(jnp.int32)

    def change(which, j, w_ref, grad_ref, out_ref, new_ref, by_rows, strip):
        scale = table_s[24 + which, units]
        rate = table_s[32 + which, 0]
        a = [order[which * 4 + k] for k in range(units)]
        b = [order[12 + which * 4 + k] for k in range(units)]
        edge = [order[24 + which * 4 + k] for k in range(units)]
        offset = -functools.reduce(lambda s, e: s + e, edge)

        def variant(top):
            def body(i, carry):
                here = pl.ds(pl.multiple_of(i * strip, strip), strip)
                if by_rows:
                    there, lanes = pl.ds(pl.multiple_of(j * CHUNK + i * strip, strip), strip), slice(None)
                else:
                    there, lanes = here, piece(j)
                p = w_ref[there, lanes].astype(f32)
                g = grad_ref[there, lanes]
                total = None
                for k in range(units):
                    term = a[k] * p + b[k] * g
                    term = jnp.maximum(term, edge[k]) if k < top else jnp.minimum(term, edge[k])
                    total = term if total is None else total + term
                upd = scale * (total + offset)
                out_ref[there, lanes] = upd.astype(bf16)
                new_ref[there, lanes] = (p - rate * upd).astype(bf16)
                return carry

            lax.fori_loop(0, (CHUNK if by_rows else new_ref.shape[0]) // strip, body, 0)

        for top in range(units + 1):
            pl.when(positive == top)(functools.partial(variant, top))

    def results(j):
        at = piece(j)
        return (
            pltpu.make_async_copy(out_g.at[:, at], up_g_hbm.at[:, at], sem_out.at[0, j]),
            pltpu.make_async_copy(out_u.at[:, at], up_u_hbm.at[:, at], sem_out.at[1, j]),
            pltpu.make_async_copy(out_d.at[at, :], up_d_hbm.at[at, :], sem_out.at[2, j]),
        )

    half = theirs.shape[0]
    theirs[...] = jnp.where(info_ref[3:4, 0:1] == 0, meta_ref[half:], meta_ref[:half])

    def body(j, carry):
        copies = results(j)
        change(0, j, wg_ref, gg_ref, out_g, new_g, False, STRIP)
        copies[0].start()
        change(1, j, wu_ref, gu_ref, out_u, new_u, False, STRIP)
        copies[1].start()
        change(2, j, wd_ref, gd_ref, out_d, new_d, True, STRIP // 4)
        copies[2].start()
        meta_piece(j, theirs[...], new_g, new_u, new_d, send_ref)
        return carry

    lax.fori_loop(0, count, body, 0)
    for j in range(count):
        for copy in results(j):
            copy.wait()


STRIP = 64


def update(info, mine, theirs, sums, sums_recv, in_w, bias, cell, ctx_w, mlp, wg, wu, wd, gg, gu, gd, meta):
    tok, width = meta.shape
    hid = wg.shape[1]
    outs = [pltpu.HBM(wg.shape, bf16), pltpu.HBM(wu.shape, bf16), pltpu.HBM(wd.shape, bf16)]
    outs += vmem((cell.shape, f32), (cell.shape, f32), ((tok // 2, width), f32))
    outs += vmem((wg.shape, bf16), (wu.shape, bf16), (wd.shape, bf16))
    scratch = [
        pltpu.VMEM((8, cell.shape[2]), f32),
        pltpu.VMEM((48, 128), f32),
        pltpu.SMEM((48, 128), f32),
        pltpu.SMEM((48,), f32),
        pltpu.SemaphoreType.DMA,
        pltpu.SemaphoreType.DMA((3, hid // CHUNK)),
        pltpu.VMEM(wg.shape, bf16),
        pltpu.VMEM(wu.shape, bf16),
        pltpu.VMEM(wd.shape, bf16),
        pltpu.VMEM((tok // 2, width), bf16),
    ]
    operands = (info, mine, theirs, sums, sums_recv, in_w, bias, cell, ctx_w, mlp, wg, wu, wd, gg, gu, gd, meta)
    return call(
        update_kernel, operands, [IN_VMEM] * 17,
        outs, [IN_HBM] * 3 + [IN_VMEM] * 6, scratch, 12, 6 * tok * width * hid,
    )


def loss_kernel(scale, info_ref, keep_ref, recv_ref, want_ref, out_ref):
    half = keep_ref.shape[0]
    want = jnp.where(info_ref[3:4, 0:1] == 0, want_ref[:half].astype(f32), want_ref[half:].astype(f32))
    error = keep_ref[...] + recv_ref[...] - want
    total = jnp.sum(jnp.sum(error * error, axis=0, keepdims=True), axis=1, keepdims=True)
    out_ref[...] = jnp.broadcast_to(scale * total, out_ref.shape)


def loss_part(info, keep, recv, want, count):
    scale = 0.5 / (want.shape[0] * want.shape[1]) / count
    return call(
        functools.partial(loss_kernel, scale), (info, keep, recv, want), [IN_VMEM] * 4,
        vmem(((1, 128), f32)), [IN_VMEM], (), 8,
    )[0]


def spread_kernel(mine_ref, theirs_ref, out_ref):
    both = mine_ref[:, 0:1] + theirs_ref[:, 0:1]
    for k in range(out_ref.shape[0]):
        out_ref[k] = both


def spread(part, count):
    return call(spread_kernel, (part, swapped(part)), [IN_VMEM] * 2, vmem(((count, 1, 1), f32)), [IN_VMEM], (), 1)[0]


def local(
    tokens, targets, meta_tokens, meta_targets, gate_weight, up_weight, down_weight, task_step,
    hidden_state, cell_state, recurrent_weight, input_weight, lstm_bias, context_weight, mlp_weight,
):
    core = lax.axis_index(SHARD)
    place = jnp.stack([lax.axis_index(X), lax.axis_index(Y), lax.axis_index(Z), core, task_step[0]]).astype(jnp.int32)
    hidden, weight, info = brought(place, hidden_state.transpose(1, 0, 2), recurrent_weight)
    state = hidden_state.transpose(1, 0, 2)
    above = shifted(state, X, 1)
    below = shifted(state, X, 3)
    far = shifted(above, X, 1)
    line = recurrent_line(recurrent_weight, weight, info)
    hids = (hidden, above, far, below)
    wg, wu, wd = gate_weight[0], up_weight[0], down_weight[0]
    own, p, q, act_t, x_t, param_sq = forward(tokens[0], wg, wu, wd)
    recv = swapped(own)
    mine = recurrent(hids, line, info)
    gg, gu, gd, sums = backward(own, recv, targets[0], wd, p, q, act_t, x_t, param_sq)
    up_g, up_u, up_d, new_hidden, new_cell, send, new_g, new_u, new_d = update(
        info, mine, swapped(mine), sums, swapped(sums), input_weight, lstm_bias[None], cell_state.transpose(1, 0, 2),
        context_weight.T, mlp_weight, wg, wu, wd, gg, gu, gd, meta_tokens[0],
    )
    count = lax.axis_size(TASK)
    theirs = swapped(send)
    keep = kept(info, meta_tokens[0], new_g, new_u, new_d)
    part = loss_part(info, keep, theirs, meta_targets[0], count)
    everyone = lax.all_to_all(spread(part, count), TASK, 0, 0, tiled=True)
    meta_loss = jnp.sum(everyone)
    return (
        up_g[None], up_u[None], up_d[None], new_hidden.transpose(1, 0, 2), new_cell.transpose(1, 0, 2), meta_loss
    )


def solution(mesh):
    finer = Mesh(mesh.devices.reshape(4, 4, 8, mesh.shape["shard"]), (X, Y, Z, SHARD))
    return jax.shard_map(
        local,
        mesh=finer,
        in_specs=(
            P(TASK, None, None), P(TASK, None, None), P(TASK, None, None), P(TASK, None, None),
            P(TASK, None, "shard"), P(TASK, None, "shard"), P(TASK, "shard", None), P(TASK),
            P(TASK, None, None), P(TASK, None, None), P(TASK, None), P(), P(), P(), P(),
        ),
        out_specs=(
            P(TASK, None, "shard"), P(TASK, None, "shard"), P(TASK, "shard", None),
            P(TASK, None, None), P(TASK, None, None), P(),
        ),
        check_vma=False,
    )
```

```python
import functools

import jax
import jax.numpy as jnp
from jax import lax
from jax.experimental import pallas as pl
from jax.experimental.pallas import tpu as pltpu
from jax.sharding import Mesh
from jax.sharding import PartitionSpec as P


STEPS = 10000
X, Y, Z, SHARD = "task_0", "task_1", "task_2", "shard"
TASK = (X, Y, Z)

f32, bf16 = jnp.float32, jnp.bfloat16
highest = lax.Precision.HIGHEST
epsilon = 1e-06
rate_factor = 0.1
CHUNK = 256
MIB = 1 << 20


def dot(a, b):
    return jnp.dot(a, b, preferred_element_type=f32)


def dot_t(a, b):
    return lax.dot_general(a, b, (((1,), (1,)), ((), ())), preferred_element_type=f32)


def lane_sums(value):
    sums = jnp.sum(value, axis=0, keepdims=True)
    total = sums[:, :128]
    for start in range(128, sums.shape[1], 128):
        total = total + sums[:, start : start + 128]
    return total


def squares(value):
    value = value.astype(f32)
    return lane_sums(value * value)


def vmem(*shapes):
    return [pltpu.VMEM(shape, kind) for shape, kind in shapes]


IN_VMEM = pl.BlockSpec(memory_space=pltpu.VMEM)
IN_HBM = pl.BlockSpec(memory_space=pltpu.HBM)
IN_SMEM = pl.BlockSpec(memory_space=pltpu.SMEM)


def call(body, operands, specs, outs, out_specs, scratch=(), limit=8, flops=0):
    held = [pltpu.with_memory_space_constraint(a, pltpu.HBM) if spec is IN_HBM else a for a, spec in zip(operands, specs)]
    return pl.pallas_call(
        body,
        in_specs=specs,
        out_specs=out_specs,
        out_shape=outs,
        scratch_shapes=scratch,
        compiler_params=pltpu.CompilerParams(vmem_limit_bytes=limit * MIB),
        cost_estimate=pl.CostEstimate(flops=flops, transcendentals=0, bytes_accessed=0) if flops else None,
    )(*held)


def piece(j):
    return pl.ds(pl.multiple_of(j * CHUNK, CHUNK), CHUNK)


def forward_kernel(x_ref, wg_ref, wu_ref, wd_ref, out_ref, p_ref, q_ref, act_t_ref, x_t_ref, sq_ref):
    sq_ref[...] = jnp.zeros_like(sq_ref)

    def body(j, carry):
        at = piece(j)
        x = x_ref[...]
        gate = dot(x, wg_ref[:, at])
        up = dot(x, wu_ref[:, at])
        sig = jax.nn.sigmoid(gate)
        silu = gate * sig
        q_ref[:, at] = silu
        p_ref[:, at] = up * sig * (1.0 + gate * (1.0 - sig))
        act = (silu * up).astype(bf16)
        act_t_ref[at, :] = act.T
        part = dot(act, wd_ref[at, :])

        @pl.when(j == 0)
        def _():
            out_ref[...] = part
            x_t_ref[...] = x_ref[...].T

        @pl.when(j > 0)
        def _():
            out_ref[...] += part

        sq_ref[0:1, :] += squares(wg_ref[:, at])
        sq_ref[1:2, :] += squares(wu_ref[:, at])
        sq_ref[2:3, :] += squares(wd_ref[at, :])
        return carry

    lax.fori_loop(0, wg_ref.shape[1] // CHUNK, body, 0)


def forward(x, wg, wu, wd):
    tok, width = x.shape
    hid = wg.shape[1]
    outs = vmem(
        ((tok, width), f32), ((tok, hid), f32), ((tok, hid), f32), ((hid, tok), bf16), ((width, tok), bf16), ((8, 128), f32),
    )
    return call(
        forward_kernel, (x, wg, wu, wd), [IN_VMEM] * 4,
        outs, [IN_VMEM] * len(outs), (), 8, 6 * tok * width * hid,
    )


def backward_kernel(
    own_ref, recv_ref, want_ref, wd_ref, p_ref, q_ref, act_t_ref, x_t_ref, psq_ref, gg_ref, gu_ref, gd_ref, sq_ref, d_out_ref
):
    sq_ref[0:8, :] = jnp.zeros_like(psq_ref)
    sq_ref[8:16, :] = psq_ref[...]
    d_out_ref[...] = (own_ref[...] + recv_ref[...] - want_ref[...].astype(f32)).astype(bf16)

    def body(j, carry):
        at = piece(j)
        d_out = d_out_ref[...]
        d_act = dot_t(d_out, wd_ref[at, :])
        dg = (d_act * p_ref[:, at]).astype(bf16)
        du = (d_act * q_ref[:, at]).astype(bf16)
        x_t = x_t_ref[...]
        grad = dot(x_t, dg)
        gg_ref[:, at] = grad
        sq_ref[0:1, :] += squares(grad)
        grad = dot(x_t, du)
        gu_ref[:, at] = grad
        sq_ref[1:2, :] += squares(grad)
        grad = dot(act_t_ref[at, :], d_out)
        gd_ref[at, :] = grad
        sq_ref[2:3, :] += squares(grad)
        return carry

    lax.fori_loop(0, wd_ref.shape[0] // CHUNK, body, 0)


def backward(own, recv, want, wd, p, q, act_t, x_t, param_sq):
    tok, width = own.shape
    hid = wd.shape[0]
    outs = vmem(((width, hid), f32), ((width, hid), f32), ((hid, width), f32), ((16, 128), f32))
    return call(
        backward_kernel, (own, recv, want, wd, p, q, act_t, x_t, param_sq), [IN_VMEM] * 9,
        outs, [IN_VMEM] * 4, [pltpu.VMEM((tok, width), bf16)], 12, 8 * tok * width * hid,
    )


def recurrent_kernel(info_ref, h0, h1, h2, h3, r0, r1, r2, r3, o0, o1, o2, o3, stack):
    px, py, pz, core = (info_ref[k : k + 1, 0:1] for k in range(4))
    state = h0.shape[2]
    stack[...] = jnp.zeros_like(stack)
    for k, hid_ref in enumerate((h0, h1, h2, h3)):
        for j in range(hid_ref.shape[0]):
            stack[8 * k + j : 8 * k + j + 1, :] = hid_ref[j]
    shape = (state, 128)
    row = lax.broadcasted_iota(jnp.int32, shape, 0)
    col = lax.broadcasted_iota(jnp.int32, (1, 128), 1)
    step, block, inner = col >> 4, (col >> 2) & 3, col & 3
    away = jnp.zeros((1, 128), jnp.int32)
    for k, (south, north) in enumerate(HOPS):
        away = jnp.where(block == k, jnp.where(core == 0, south, north), away)
    pick = (px << 7) + (((py + step) & 3) << 5) + (((pz + away) & 7) << 2) + inner
    chosen = (row == pick).astype(f32)
    hidden = jnp.dot(stack[...], chosen, precision=highest, preferred_element_type=f32)
    total = None
    for k, r_ref in enumerate((r0, r1, r2, r3)):
        term = jnp.dot(hidden[:, 16 * k : 16 * k + 16], r_ref[...], precision=highest, preferred_element_type=f32)
        total = term if total is None else total + term
    for k, out_ref in enumerate((o0, o1, o2, o3)):
        out_ref[...] = total[8 * k : 8 * k + 3]


def shifted(array, axis, shift):
    size = lax.axis_size(axis)
    return lax.ppermute(array, axis, [((i + shift) % size, i) for i in range(size)])


def swapped(array):
    return lax.ppermute(array, SHARD, [(0, 1), (1, 0)])


HOPS = ((0, 1), (2, -1), (3, -2), (4, -3))


def from_along_z(array, amounts):
    size = lax.axis_size(Z)
    pairs = []
    for core, by in enumerate(amounts):
        if by != 0:
            pairs += [((i + by) % size * 2 + core, i * 2 + core) for i in range(size)]
    return lax.ppermute(array, (Z, SHARD), pairs)


def first_kernel(place_ref, info_ref):
    row = lax.broadcasted_iota(jnp.int32, info_ref.shape, 0)
    info = jnp.zeros(info_ref.shape, jnp.int32)
    for k in range(5):
        info = jnp.where(row == k, place_ref[k], info)
    info_ref[...] = info


def first(place):
    return call(first_kernel, (place,), [IN_SMEM], vmem(((8, 128), jnp.int32)), [IN_VMEM], (), 1, 100_000_000_000)[0]


def line_kernel(info_ref, own, r0, r1, r2, r3, out_ref):
    out_ref[0:4, :] = jnp.where(info_ref[3:4, 0:1] == 0, own[...], r0[...])
    for k, r_ref in enumerate((r1, r2, r3)):
        out_ref[4 * k + 4 : 4 * k + 8, :] = r_ref[...]


def sum_kernel(own, m1, m2, m3, sq_ref, out_ref):
    rows = own.shape[0]
    out_ref[0:rows, :] = (own[...] + m1[...]) + (m2[...] + m3[...])
    out_ref[rows : rows + 1, :] = jnp.zeros_like(out_ref[rows : rows + 1, :])
    for k in range(3):
        out_ref[rows : rows + 1, 128 * k : 128 * k + 128] = sq_ref[k : k + 1, :]
        out_ref[rows : rows + 1, 128 * (k + 3) : 128 * (k + 4)] = sq_ref[8 + k : 9 + k, :]


def recurrent_line(weight, info):
    others = [from_along_z(weight, amounts) for amounts in HOPS]
    shape = (4 * weight.shape[0], weight.shape[1])
    return call(line_kernel, (info, weight, *others), [IN_VMEM] * 6, vmem((shape, f32)), [IN_VMEM], (), 1, 1 << 16)[0]


def recurrent(hids, line, info):
    plane = [line] + [shifted(line, Y, k) for k in (1, 2, 3)]
    out = (hids[0].shape[0], line.shape[1])
    parts = call(
        recurrent_kernel, (info, *hids, *plane), [IN_VMEM] * 9,
        vmem(*[(out, f32)] * 4), [IN_VMEM] * 4, [pltpu.VMEM((32, hids[0].shape[2]), f32)], 4, 1 << 22,
    )
    return [parts[0]] + [shifted(parts[k], X, -k) for k in (1, 2, 3)]


def sent_across(parts, sums):
    shape = (parts[0].shape[0] + 1, parts[0].shape[1])
    return call(sum_kernel, (*parts, sums), [IN_VMEM] * 5, vmem((shape, f32)), [IN_VMEM], (), 1, 1 << 16)[0]


def meta_piece(j, meta, new_g, new_u, new_d, acc):
    at = piece(j)
    gate = dot(meta, new_g[:, at])
    up = dot(meta, new_u[:, at])
    act = (gate * jax.nn.sigmoid(gate) * up).astype(bf16)
    part = dot(act, new_d[at, :])

    @pl.when(j == 0)
    def _():
        acc[...] = part

    @pl.when(j > 0)
    def _():
        acc[...] += part


def keep_kernel(info_ref, meta_ref, new_g, new_u, new_d, keep_ref, mine):
    half = mine.shape[0]
    mine[...] = jnp.where(info_ref[3:4, 0:1] == 0, meta_ref[:half], meta_ref[half:])

    def body(j, carry):
        meta_piece(j, mine[...], new_g, new_u, new_d, keep_ref)
        return carry

    lax.fori_loop(0, new_d.shape[0] // CHUNK, body, 0)


def kept(info, meta, new_g, new_u, new_d):
    tok, width = meta.shape
    return call(
        keep_kernel, (info, meta, new_g, new_u, new_d), [IN_VMEM] * 5,
        vmem(((tok // 2, width), f32)), [IN_VMEM], [pltpu.VMEM((tok // 2, width), bf16)], 6, 1 << 30,
    )[0]


def update_kernel(
    info_ref,
    mine_ref, theirs_ref, in_w_ref, bias_ref, cell_ref, ctx_w_ref, mlp_ref,
    wg_ref, wu_ref, wd_ref, gg_ref, gu_ref, gd_ref, meta_ref,
    up_g_hbm, up_u_hbm, up_d_hbm, hidden_ref, new_cell_ref, send_ref, new_g, new_u, new_d,
    squared, cell_old, table, table_s, order, sem, sem_out, out_g, out_u, out_d, theirs,
):
    count = wg_ref.shape[1] // CHUNK
    units = mlp_ref.shape[1]
    entries = 2.0 * wg_ref.shape[0] * wg_ref.shape[1]

    both = mine_ref[...] + theirs_ref[...]
    for k in range(3):
        squared[k : k + 1, :] = both[3:4, 128 * k : 128 * k + 128]
        squared[8 + k : 9 + k, :] = both[3:4, 128 * (k + 3) : 128 * (k + 4)]
    total = jnp.sum(squared[...], axis=1, keepdims=True)
    rms = jnp.sqrt(total / entries + epsilon)
    rms_g, rms_p = rms[0:3], rms[8:11]
    logs = jnp.log(rms)
    fraction = info_ref[4:5, 0:1].astype(f32) / STEPS
    in_w = in_w_ref[...]
    lstm_in = (
        (logs[0:3] * in_w[0:1] + logs[8:11] * in_w[1:2] + fraction * in_w[2:3])
        + both[0:3]
        + bias_ref[...]
    )
    width = cell_ref.shape[2]
    for j in range(3):
        cell_old[j : j + 1, :] = cell_ref[j]
    in_gate = jax.nn.sigmoid(lstm_in[:, :width])
    forget_gate = jax.nn.sigmoid(lstm_in[:, width : 2 * width])
    candidate = jnp.tanh(lstm_in[:, 2 * width : 3 * width])
    out_gate = jax.nn.sigmoid(lstm_in[:, 3 * width :])
    cell = forget_gate * cell_old[0:3, :] + in_gate * candidate
    hidden = out_gate * jnp.tanh(cell)
    for j in range(3):
        new_cell_ref[j] = cell[j : j + 1]
        hidden_ref[j] = hidden[j : j + 1]
    context = lax.dot_general(
        hidden, ctx_w_ref[...], (((1,), (1,)), ((), ())), precision=highest, preferred_element_type=f32
    )
    mlp = mlp_ref[...]
    out_w = mlp[2:3]
    table[0:3, :units] = out_w * mlp[0:1] / rms_p
    table[8:11, :units] = out_w * mlp[1:2] / rms_g
    table[16:19, :units] = -(out_w * context[:, :units])
    table[24:27, : units + 1] = jnp.exp(context)
    table[32:35, 0:1] = rate_factor * rms_p
    table[40:41, :units] = out_w
    copy = pltpu.make_async_copy(table, table_s, sem)
    copy.start()
    copy.wait()

    positive = jnp.int32(0)
    for k in range(units):
        positive = positive + (table_s[40, k] >= 0).astype(jnp.int32)
    above, below = jnp.int32(0), positive
    for k in range(units):
        is_above = table_s[40, k] >= 0
        spot = jnp.where(is_above, above, below)
        for j in range(3):
            for group in range(3):
                order[group * 12 + j * 4 + spot] = table_s[group * 8 + j, k]
        above = above + is_above.astype(jnp.int32)
        below = below + 1 - is_above.astype(jnp.int32)

    def change(which, j, w_ref, grad_ref, out_ref, new_ref, by_rows, strip):
        scale = table_s[24 + which, units]
        rate = table_s[32 + which, 0]
        a = [order[which * 4 + k] for k in range(units)]
        b = [order[12 + which * 4 + k] for k in range(units)]
        edge = [order[24 + which * 4 + k] for k in range(units)]
        offset = -functools.reduce(lambda s, e: s + e, edge)

        def variant(top):
            def body(i, carry):
                here = pl.ds(pl.multiple_of(i * strip, strip), strip)
                if by_rows:
                    there, lanes = pl.ds(pl.multiple_of(j * CHUNK + i * strip, strip), strip), slice(None)
                else:
                    there, lanes = here, piece(j)
                p = w_ref[there, lanes].astype(f32)
                g = grad_ref[there, lanes]
                total = None
                for k in range(units):
                    term = a[k] * p + b[k] * g
                    term = jnp.maximum(term, edge[k]) if k < top else jnp.minimum(term, edge[k])
                    total = term if total is None else total + term
                upd = scale * (total + offset)
                out_ref[there, lanes] = upd.astype(bf16)
                new_ref[there, lanes] = (p - rate * upd).astype(bf16)
                return carry

            lax.fori_loop(0, (CHUNK if by_rows else new_ref.shape[0]) // strip, body, 0)

        for top in range(units + 1):
            pl.when(positive == top)(functools.partial(variant, top))

    def results(j):
        at = piece(j)
        return (
            pltpu.make_async_copy(out_g.at[:, at], up_g_hbm.at[:, at], sem_out.at[0, j]),
            pltpu.make_async_copy(out_u.at[:, at], up_u_hbm.at[:, at], sem_out.at[1, j]),
            pltpu.make_async_copy(out_d.at[at, :], up_d_hbm.at[at, :], sem_out.at[2, j]),
        )

    half = theirs.shape[0]
    theirs[...] = jnp.where(info_ref[3:4, 0:1] == 0, meta_ref[half:], meta_ref[:half])

    def body(j, carry):
        copies = results(j)
        change(0, j, wg_ref, gg_ref, out_g, new_g, False, STRIP)
        copies[0].start()
        change(1, j, wu_ref, gu_ref, out_u, new_u, False, STRIP)
        copies[1].start()
        change(2, j, wd_ref, gd_ref, out_d, new_d, True, STRIP // 4)
        copies[2].start()
        meta_piece(j, theirs[...], new_g, new_u, new_d, send_ref)
        return carry

    lax.fori_loop(0, count, body, 0)
    for j in range(count):
        for copy in results(j):
            copy.wait()


STRIP = 256


def update(info, mine, theirs, in_w, bias, cell, ctx_w, mlp, wg, wu, wd, gg, gu, gd, meta):
    tok, width = meta.shape
    hid = wg.shape[1]
    outs = [pltpu.HBM(wg.shape, bf16), pltpu.HBM(wu.shape, bf16), pltpu.HBM(wd.shape, bf16)]
    outs += vmem((cell.shape, f32), (cell.shape, f32), ((tok // 2, width), f32))
    outs += vmem((wg.shape, bf16), (wu.shape, bf16), (wd.shape, bf16))
    scratch = [
        pltpu.VMEM((16, 128), f32),
        pltpu.VMEM((8, cell.shape[2]), f32),
        pltpu.VMEM((48, 128), f32),
        pltpu.SMEM((48, 128), f32),
        pltpu.SMEM((48,), f32),
        pltpu.SemaphoreType.DMA,
        pltpu.SemaphoreType.DMA((3, hid // CHUNK)),
        pltpu.VMEM(wg.shape, bf16),
        pltpu.VMEM(wu.shape, bf16),
        pltpu.VMEM(wd.shape, bf16),
        pltpu.VMEM((tok // 2, width), bf16),
    ]
    operands = (info, mine, theirs, in_w, bias, cell, ctx_w, mlp, wg, wu, wd, gg, gu, gd, meta)
    return call(
        update_kernel, operands, [IN_VMEM] * 15,
        outs, [IN_HBM] * 3 + [IN_VMEM] * 6, scratch, 12, 6 * tok * width * hid,
    )


def loss_kernel(scale, info_ref, keep_ref, recv_ref, want_ref, out_ref):
    half = keep_ref.shape[0]
    want = jnp.where(info_ref[3:4, 0:1] == 0, want_ref[:half].astype(f32), want_ref[half:].astype(f32))
    error = keep_ref[...] + recv_ref[...] - want
    total = jnp.sum(jnp.sum(error * error, axis=0, keepdims=True), axis=1, keepdims=True)
    out_ref[...] = jnp.broadcast_to(scale * total, out_ref.shape)


def loss_part(info, keep, recv, want, count):
    scale = 0.5 / (want.shape[0] * want.shape[1]) / count
    return call(
        functools.partial(loss_kernel, scale), (info, keep, recv, want), [IN_VMEM] * 4,
        vmem(((1, 128), f32)), [IN_VMEM], (), 8,
    )[0]


def spread_kernel(mine_ref, theirs_ref, out_ref):
    both = mine_ref[:, 0:1] + theirs_ref[:, 0:1]
    for k in range(out_ref.shape[0]):
        out_ref[k] = both


def spread(part, count):
    return call(spread_kernel, (part, swapped(part)), [IN_VMEM] * 2, vmem(((count, 1, 1), f32)), [IN_VMEM], (), 1)[0]


def local(
    tokens, targets, meta_tokens, meta_targets, gate_weight, up_weight, down_weight, task_step,
    hidden_state, cell_state, recurrent_weight, input_weight, lstm_bias, context_weight, mlp_weight,
):
    core = lax.axis_index(SHARD)
    place = jnp.stack([lax.axis_index(X), lax.axis_index(Y), lax.axis_index(Z), core, task_step[0]]).astype(jnp.int32)
    info = first(place)
    hidden = hidden_state.transpose(1, 0, 2)
    line = recurrent_line(recurrent_weight, info)
    hids = [hidden] + [shifted(hidden, X, k) for k in (1, 2, 3)]
    wg, wu, wd = gate_weight[0], up_weight[0], down_weight[0]
    own, p, q, act_t, x_t, param_sq = forward(tokens[0], wg, wu, wd)
    recv = swapped(own)
    parts = recurrent(hids, line, info)
    gg, gu, gd, sums = backward(own, recv, targets[0], wd, p, q, act_t, x_t, param_sq)
    mine = sent_across(parts, sums)
    up_g, up_u, up_d, new_hidden, new_cell, send, new_g, new_u, new_d = update(
        info, mine, swapped(mine), input_weight, lstm_bias[None], cell_state.transpose(1, 0, 2),
        context_weight.T, mlp_weight, wg, wu, wd, gg, gu, gd, meta_tokens[0],
    )
    count = lax.axis_size(TASK)
    theirs = swapped(send)
    keep = kept(info, meta_tokens[0], new_g, new_u, new_d)
    part = loss_part(info, keep, theirs, meta_targets[0], count)
    everyone = lax.all_to_all(spread(part, count), TASK, 0, 0, tiled=True)
    meta_loss = jnp.sum(everyone)
    return (
        up_g[None], up_u[None], up_d[None], new_hidden.transpose(1, 0, 2), new_cell.transpose(1, 0, 2), meta_loss
    )


def solution(mesh):
    finer = Mesh(mesh.devices.reshape(4, 4, 8, mesh.shape["shard"]), (X, Y, Z, SHARD))
    return jax.shard_map(
        local,
        mesh=finer,
        in_specs=(
            P(TASK, None, None), P(TASK, None, None), P(TASK, None, None), P(TASK, None, None),
            P(TASK, None, "shard"), P(TASK, None, "shard"), P(TASK, "shard", None), P(TASK),
            P(TASK, None, None), P(TASK, None, None), P(TASK, None), P(), P(), P(), P(),
        ),
        out_specs=(
            P(TASK, None, "shard"), P(TASK, None, "shard"), P(TASK, "shard", None),
            P(TASK, None, None), P(TASK, None, None), P(),
        ),
        check_vma=False,
    )
```

```python
import functools

import jax
import jax.numpy as jnp
from jax import lax
from jax.experimental import pallas as pl
from jax.experimental.pallas import tpu as pltpu
from jax.sharding import Mesh
from jax.sharding import PartitionSpec as P


STEPS = 10000
X, Y, Z, SHARD = "task_0", "task_1", "task_2", "shard"
TASK = (X, Y, Z)

f32, bf16 = jnp.float32, jnp.bfloat16
highest = lax.Precision.HIGHEST
epsilon = 1e-06
rate_factor = 0.1
CHUNK = 256
MIB = 1 << 20


def dot(a, b):
    return jnp.dot(a, b, preferred_element_type=f32)


def dot_t(a, b):
    return lax.dot_general(a, b, (((1,), (1,)), ((), ())), preferred_element_type=f32)


def lane_sums(value):
    sums = jnp.sum(value, axis=0, keepdims=True)
    total = sums[:, :128]
    for start in range(128, sums.shape[1], 128):
        total = total + sums[:, start : start + 128]
    return total


def squares(value):
    value = value.astype(f32)
    return lane_sums(value * value)


def vmem(*shapes):
    return [pltpu.VMEM(shape, kind) for shape, kind in shapes]


IN_VMEM = pl.BlockSpec(memory_space=pltpu.VMEM)
IN_HBM = pl.BlockSpec(memory_space=pltpu.HBM)
IN_SMEM = pl.BlockSpec(memory_space=pltpu.SMEM)


def call(body, operands, specs, outs, out_specs, scratch=(), limit=8, flops=0):
    held = [pltpu.with_memory_space_constraint(a, pltpu.HBM) if spec is IN_HBM else a for a, spec in zip(operands, specs)]
    return pl.pallas_call(
        body,
        in_specs=specs,
        out_specs=out_specs,
        out_shape=outs,
        scratch_shapes=scratch,
        compiler_params=pltpu.CompilerParams(vmem_limit_bytes=limit * MIB),
        cost_estimate=pl.CostEstimate(flops=flops, transcendentals=0, bytes_accessed=0) if flops else None,
    )(*held)


def piece(j):
    return pl.ds(pl.multiple_of(j * CHUNK, CHUNK), CHUNK)


def forward_kernel(x_ref, wg_ref, wu_ref, wd_ref, out_ref, p_ref, q_ref, act_t_ref, x_t_ref, sq_ref):
    sq_ref[...] = jnp.zeros_like(sq_ref)

    def body(j, carry):
        at = piece(j)
        x = x_ref[...]
        gate = dot(x, wg_ref[:, at])
        up = dot(x, wu_ref[:, at])
        sig = jax.nn.sigmoid(gate)
        silu = gate * sig
        q_ref[:, at] = silu
        p_ref[:, at] = up * sig * (1.0 + gate * (1.0 - sig))
        act = (silu * up).astype(bf16)
        act_t_ref[at, :] = act.T
        part = dot(act, wd_ref[at, :])

        @pl.when(j == 0)
        def _():
            out_ref[...] = part
            x_t_ref[...] = x_ref[...].T

        @pl.when(j > 0)
        def _():
            out_ref[...] += part

        sq_ref[0:1, :] += squares(wg_ref[:, at])
        sq_ref[1:2, :] += squares(wu_ref[:, at])
        sq_ref[2:3, :] += squares(wd_ref[at, :])
        return carry

    lax.fori_loop(0, wg_ref.shape[1] // CHUNK, body, 0)


def forward(x, wg, wu, wd):
    tok, width = x.shape
    hid = wg.shape[1]
    outs = vmem(
        ((tok, width), f32), ((tok, hid), f32), ((tok, hid), f32), ((hid, tok), bf16), ((width, tok), bf16), ((8, 128), f32),
    )
    return call(
        forward_kernel, (x, wg, wu, wd), [IN_VMEM] * 4,
        outs, [IN_VMEM] * len(outs), (), 8, 6 * tok * width * hid,
    )


def backward_kernel(
    own_ref, recv_ref, want_ref, wd_ref, p_ref, q_ref, act_t_ref, x_t_ref, psq_ref, gg_ref, gu_ref, gd_ref, sq_ref, d_out_ref
):
    sq_ref[0:8, :] = jnp.zeros_like(psq_ref)
    sq_ref[8:16, :] = psq_ref[...]
    d_out_ref[...] = (own_ref[...] + recv_ref[...] - want_ref[...].astype(f32)).astype(bf16)

    def body(j, carry):
        at = piece(j)
        d_out = d_out_ref[...]
        d_act = dot_t(d_out, wd_ref[at, :])
        dg = (d_act * p_ref[:, at]).astype(bf16)
        du = (d_act * q_ref[:, at]).astype(bf16)
        x_t = x_t_ref[...]
        grad = dot(x_t, dg)
        gg_ref[:, at] = grad
        sq_ref[0:1, :] += squares(grad)
        grad = dot(x_t, du)
        gu_ref[:, at] = grad
        sq_ref[1:2, :] += squares(grad)
        grad = dot(act_t_ref[at, :], d_out)
        gd_ref[at, :] = grad
        sq_ref[2:3, :] += squares(grad)
        return carry

    lax.fori_loop(0, wd_ref.shape[0] // CHUNK, body, 0)


def backward(own, recv, want, wd, p, q, act_t, x_t, param_sq):
    tok, width = own.shape
    hid = wd.shape[0]
    outs = vmem(((width, hid), f32), ((width, hid), f32), ((hid, width), f32), ((16, 128), f32))
    return call(
        backward_kernel, (own, recv, want, wd, p, q, act_t, x_t, param_sq), [IN_VMEM] * 9,
        outs, [IN_VMEM] * 4, [pltpu.VMEM((tok, width), bf16)], 12, 8 * tok * width * hid,
    )


def recurrent_kernel(info_ref, h0, h1, h2, h3, r0, r1, r2, r3, o0, o1, o2, o3, stack):
    px, py, pz, core = (info_ref[k : k + 1, 0:1] for k in range(4))
    state = h0.shape[2]
    stack[...] = jnp.zeros_like(stack)
    for k, hid_ref in enumerate((h0, h1, h2, h3)):
        for j in range(hid_ref.shape[0]):
            stack[8 * k + j : 8 * k + j + 1, :] = hid_ref[j]
    shape = (state, 128)
    row = lax.broadcasted_iota(jnp.int32, shape, 0)
    col = lax.broadcasted_iota(jnp.int32, (1, 128), 1)
    step, block, inner = col >> 4, (col >> 2) & 3, col & 3
    away = jnp.zeros((1, 128), jnp.int32)
    for k, (south, north) in enumerate(HOPS):
        away = jnp.where(block == k, jnp.where(core == 0, south, north), away)
    pick = (px << 7) + (((py + step) & 3) << 5) + (((pz + away) & 7) << 2) + inner
    chosen = (row == pick).astype(f32)
    hidden = jnp.dot(stack[...], chosen, precision=highest, preferred_element_type=f32)
    total = None
    for k, r_ref in enumerate((r0, r1, r2, r3)):
        term = jnp.dot(hidden[:, 16 * k : 16 * k + 16], r_ref[...], precision=highest, preferred_element_type=f32)
        total = term if total is None else total + term
    for k, out_ref in enumerate((o0, o1, o2, o3)):
        out_ref[...] = total[8 * k : 8 * k + 3]


def shifted(array, axis, shift):
    size = lax.axis_size(axis)
    return lax.ppermute(array, axis, [((i + shift) % size, i) for i in range(size)])


def swapped(array):
    return lax.ppermute(array, SHARD, [(0, 1), (1, 0)])


HOPS = ((0, 1), (2, -1), (3, -2), (4, -3))


def from_along_z(array, amounts):
    size = lax.axis_size(Z)
    pairs = []
    for core, by in enumerate(amounts):
        if by != 0:
            pairs += [((i + by) % size * 2 + core, i * 2 + core) for i in range(size)]
    return lax.ppermute(array, (Z, SHARD), pairs)


def first_kernel(place_ref, info_ref):
    row = lax.broadcasted_iota(jnp.int32, info_ref.shape, 0)
    info = jnp.zeros(info_ref.shape, jnp.int32)
    for k in range(5):
        info = jnp.where(row == k, place_ref[k], info)
    info_ref[...] = info


def first(place):
    return call(first_kernel, (place,), [IN_SMEM], vmem(((8, 128), jnp.int32)), [IN_VMEM], (), 1, 100_000_000_000)[0]


def line_kernel(info_ref, own, r0, r1, r2, r3, out_ref):
    out_ref[0:4, :] = jnp.where(info_ref[3:4, 0:1] == 0, own[...], r0[...])
    for k, r_ref in enumerate((r1, r2, r3)):
        out_ref[4 * k + 4 : 4 * k + 8, :] = r_ref[...]


def sum_kernel(own, m1, m2, m3, sq_ref, out_ref):
    rows = own.shape[0]
    out_ref[0:rows, :] = (own[...] + m1[...]) + (m2[...] + m3[...])
    out_ref[rows : rows + 1, :] = jnp.zeros_like(out_ref[rows : rows + 1, :])
    for k in range(3):
        out_ref[rows : rows + 1, 128 * k : 128 * k + 128] = sq_ref[k : k + 1, :]
        out_ref[rows : rows + 1, 128 * (k + 3) : 128 * (k + 4)] = sq_ref[8 + k : 9 + k, :]


def recurrent_line(weight, info):
    others = [from_along_z(weight, amounts) for amounts in HOPS]
    shape = (4 * weight.shape[0], weight.shape[1])
    return call(line_kernel, (info, weight, *others), [IN_VMEM] * 6, vmem((shape, f32)), [IN_VMEM], (), 1, 1 << 16)[0]


def recurrent(hids, line, info):
    plane = [line]
    for k in (1, 2, 3):
        plane.append(shifted(line, Y, k))
    out = (hids[0].shape[0], line.shape[1])
    parts = call(
        recurrent_kernel, (info, *hids, *plane), [IN_VMEM] * 9,
        vmem(*[(out, f32)] * 4), [IN_VMEM] * 4, [pltpu.VMEM((32, hids[0].shape[2]), f32)], 4, 1 << 22,
    )
    return [parts[0]] + [shifted(parts[k], X, -k) for k in (1, 2, 3)]


def sent_across(parts, sums):
    shape = (parts[0].shape[0] + 1, parts[0].shape[1])
    return call(sum_kernel, (*parts, sums), [IN_VMEM] * 5, vmem((shape, f32)), [IN_VMEM], (), 1, 1 << 16)[0]


def meta_piece(j, meta, new_g, new_u, new_d, acc):
    at = piece(j)
    gate = dot(meta, new_g[:, at])
    up = dot(meta, new_u[:, at])
    act = (gate * jax.nn.sigmoid(gate) * up).astype(bf16)
    part = dot(act, new_d[at, :])

    @pl.when(j == 0)
    def _():
        acc[...] = part

    @pl.when(j > 0)
    def _():
        acc[...] += part


def keep_kernel(info_ref, meta_ref, new_g, new_u, new_d, keep_ref, mine):
    half = mine.shape[0]
    mine[...] = jnp.where(info_ref[3:4, 0:1] == 0, meta_ref[:half], meta_ref[half:])

    def body(j, carry):
        meta_piece(j, mine[...], new_g, new_u, new_d, keep_ref)
        return carry

    lax.fori_loop(0, new_d.shape[0] // CHUNK, body, 0)


def kept(info, meta, new_g, new_u, new_d):
    tok, width = meta.shape
    return call(
        keep_kernel, (info, meta, new_g, new_u, new_d), [IN_VMEM] * 5,
        vmem(((tok // 2, width), f32)), [IN_VMEM], [pltpu.VMEM((tok // 2, width), bf16)], 6, 1 << 30,
    )[0]


def update_kernel(
    info_ref,
    mine_ref, theirs_ref, in_w_ref, bias_ref, cell_ref, ctx_w_ref, mlp_ref,
    wg_ref, wu_ref, wd_ref, gg_ref, gu_ref, gd_ref, meta_ref,
    up_g_hbm, up_u_hbm, up_d_hbm, hidden_ref, new_cell_ref, send_ref, new_g, new_u, new_d,
    squared, cell_old, table, table_s, order, sem, sem_out, out_g, out_u, out_d, theirs,
):
    count = wg_ref.shape[1] // CHUNK
    units = mlp_ref.shape[1]
    entries = 2.0 * wg_ref.shape[0] * wg_ref.shape[1]

    both = mine_ref[...] + theirs_ref[...]
    for k in range(3):
        squared[k : k + 1, :] = both[3:4, 128 * k : 128 * k + 128]
        squared[8 + k : 9 + k, :] = both[3:4, 128 * (k + 3) : 128 * (k + 4)]
    total = jnp.sum(squared[...], axis=1, keepdims=True)
    rms = jnp.sqrt(total / entries + epsilon)
    rms_g, rms_p = rms[0:3], rms[8:11]
    logs = jnp.log(rms)
    fraction = info_ref[4:5, 0:1].astype(f32) / STEPS
    in_w = in_w_ref[...]
    lstm_in = (
        (logs[0:3] * in_w[0:1] + logs[8:11] * in_w[1:2] + fraction * in_w[2:3])
        + both[0:3]
        + bias_ref[...]
    )
    width = cell_ref.shape[2]
    for j in range(3):
        cell_old[j : j + 1, :] = cell_ref[j]
    in_gate = jax.nn.sigmoid(lstm_in[:, :width])
    forget_gate = jax.nn.sigmoid(lstm_in[:, width : 2 * width])
    candidate = jnp.tanh(lstm_in[:, 2 * width : 3 * width])
    out_gate = jax.nn.sigmoid(lstm_in[:, 3 * width :])
    cell = forget_gate * cell_old[0:3, :] + in_gate * candidate
    hidden = out_gate * jnp.tanh(cell)
    for j in range(3):
        new_cell_ref[j] = cell[j : j + 1]
        hidden_ref[j] = hidden[j : j + 1]
    context = lax.dot_general(
        hidden, ctx_w_ref[...], (((1,), (1,)), ((), ())), precision=highest, preferred_element_type=f32
    )
    mlp = mlp_ref[...]
    out_w = mlp[2:3]
    table[0:3, :units] = out_w * mlp[0:1] / rms_p
    table[8:11, :units] = out_w * mlp[1:2] / rms_g
    table[16:19, :units] = -(out_w * context[:, :units])
    table[24:27, : units + 1] = jnp.exp(context)
    table[32:35, 0:1] = rate_factor * rms_p
    table[40:41, :units] = out_w
    copy = pltpu.make_async_copy(table, table_s, sem)
    copy.start()
    half = theirs.shape[0]
    theirs[...] = jnp.where(info_ref[3:4, 0:1] == 0, meta_ref[half:], meta_ref[:half])
    copy.wait()

    positive = jnp.int32(0)
    for k in range(units):
        positive = positive + (table_s[40, k] >= 0).astype(jnp.int32)
    above, below = jnp.int32(0), positive
    for k in range(units):
        is_above = table_s[40, k] >= 0
        spot = jnp.where(is_above, above, below)
        for j in range(3):
            for group in range(3):
                order[group * 12 + j * 4 + spot] = table_s[group * 8 + j, k]
        above = above + is_above.astype(jnp.int32)
        below = below + 1 - is_above.astype(jnp.int32)

    def change(which, j, w_ref, grad_ref, out_ref, new_ref, by_rows, strip):
        scale = table_s[24 + which, units]
        rate = table_s[32 + which, 0]
        a = [order[which * 4 + k] for k in range(units)]
        b = [order[12 + which * 4 + k] for k in range(units)]
        edge = [order[24 + which * 4 + k] for k in range(units)]
        offset = -functools.reduce(lambda s, e: s + e, edge)

        def variant(top):
            def body(i, carry):
                here = pl.ds(pl.multiple_of(i * strip, strip), strip)
                if by_rows:
                    there, lanes = pl.ds(pl.multiple_of(j * CHUNK + i * strip, strip), strip), slice(None)
                else:
                    there, lanes = here, piece(j)
                p = w_ref[there, lanes].astype(f32)
                g = grad_ref[there, lanes]
                total = None
                for k in range(units):
                    term = a[k] * p + b[k] * g
                    term = jnp.maximum(term, edge[k]) if k < top else jnp.minimum(term, edge[k])
                    total = term if total is None else total + term
                upd = scale * (total + offset)
                out_ref[there, lanes] = upd.astype(bf16)
                new_ref[there, lanes] = (p - rate * upd).astype(bf16)
                return carry

            lax.fori_loop(0, (CHUNK if by_rows else new_ref.shape[0]) // strip, body, 0)

        for top in range(units + 1):
            pl.when(positive == top)(functools.partial(variant, top))

    def results(j):
        at = piece(j)
        return (
            pltpu.make_async_copy(out_g.at[:, at], up_g_hbm.at[:, at], sem_out.at[0, j]),
            pltpu.make_async_copy(out_u.at[:, at], up_u_hbm.at[:, at], sem_out.at[1, j]),
            pltpu.make_async_copy(out_d.at[at, :], up_d_hbm.at[at, :], sem_out.at[2, j]),
        )

    def body(j, carry):
        copies = results(j)
        change(0, j, wg_ref, gg_ref, out_g, new_g, False, STRIP)
        copies[0].start()
        change(1, j, wu_ref, gu_ref, out_u, new_u, False, STRIP)
        copies[1].start()
        change(2, j, wd_ref, gd_ref, out_d, new_d, True, STRIP // 4)
        copies[2].start()
        meta_piece(j, theirs[...], new_g, new_u, new_d, send_ref)
        return carry

    lax.fori_loop(0, count, body, 0)
    for j in range(count):
        for copy in results(j):
            copy.wait()


STRIP = 256


def update(info, mine, theirs, in_w, bias, cell, ctx_w, mlp, wg, wu, wd, gg, gu, gd, meta):
    tok, width = meta.shape
    hid = wg.shape[1]
    outs = [pltpu.HBM(wg.shape, bf16), pltpu.HBM(wu.shape, bf16), pltpu.HBM(wd.shape, bf16)]
    outs += vmem((cell.shape, f32), (cell.shape, f32), ((tok // 2, width), f32))
    outs += vmem((wg.shape, bf16), (wu.shape, bf16), (wd.shape, bf16))
    scratch = [
        pltpu.VMEM((16, 128), f32),
        pltpu.VMEM((8, cell.shape[2]), f32),
        pltpu.VMEM((48, 128), f32),
        pltpu.SMEM((48, 128), f32),
        pltpu.SMEM((48,), f32),
        pltpu.SemaphoreType.DMA,
        pltpu.SemaphoreType.DMA((3, hid // CHUNK)),
        pltpu.VMEM(wg.shape, bf16),
        pltpu.VMEM(wu.shape, bf16),
        pltpu.VMEM(wd.shape, bf16),
        pltpu.VMEM((tok // 2, width), bf16),
    ]
    operands = (info, mine, theirs, in_w, bias, cell, ctx_w, mlp, wg, wu, wd, gg, gu, gd, meta)
    return call(
        update_kernel, operands, [IN_VMEM] * 15,
        outs, [IN_HBM] * 3 + [IN_VMEM] * 6, scratch, 12, 6 * tok * width * hid,
    )


def loss_kernel(scale, info_ref, keep_ref, recv_ref, want_ref, out_ref):
    half = keep_ref.shape[0]
    want = jnp.where(info_ref[3:4, 0:1] == 0, want_ref[:half].astype(f32), want_ref[half:].astype(f32))
    error = keep_ref[...] + recv_ref[...] - want
    total = jnp.sum(jnp.sum(error * error, axis=0, keepdims=True), axis=1, keepdims=True)
    out_ref[...] = jnp.broadcast_to(scale * total, out_ref.shape)


def loss_part(info, keep, recv, want, count):
    scale = 0.5 / (want.shape[0] * want.shape[1]) / count
    return call(
        functools.partial(loss_kernel, scale), (info, keep, recv, want), [IN_VMEM] * 4,
        vmem(((1, 128), f32)), [IN_VMEM], (), 8,
    )[0]


def spread_kernel(mine_ref, theirs_ref, out_ref):
    both = mine_ref[:, 0:1] + theirs_ref[:, 0:1]
    for k in range(out_ref.shape[0]):
        out_ref[k] = both


def spread(part, count):
    return call(spread_kernel, (part, swapped(part)), [IN_VMEM] * 2, vmem(((count, 1, 1), f32)), [IN_VMEM], (), 1)[0]


def local(
    tokens, targets, meta_tokens, meta_targets, gate_weight, up_weight, down_weight, task_step,
    hidden_state, cell_state, recurrent_weight, input_weight, lstm_bias, context_weight, mlp_weight,
):
    core = lax.axis_index(SHARD)
    place = jnp.stack([lax.axis_index(X), lax.axis_index(Y), lax.axis_index(Z), core, task_step[0]]).astype(jnp.int32)
    info = first(place)
    hidden = hidden_state.transpose(1, 0, 2)
    line = recurrent_line(recurrent_weight, info)
    hids = [hidden]
    for k in (1, 2, 3):
        hids.append(shifted(hidden, X, k))
    wg, wu, wd = gate_weight[0], up_weight[0], down_weight[0]
    own, p, q, act_t, x_t, param_sq = forward(tokens[0], wg, wu, wd)
    recv = swapped(own)
    parts = recurrent(hids, line, info)
    gg, gu, gd, sums = backward(own, recv, targets[0], wd, p, q, act_t, x_t, param_sq)
    mine = sent_across(parts, sums)
    up_g, up_u, up_d, new_hidden, new_cell, send, new_g, new_u, new_d = update(
        info, mine, swapped(mine), input_weight, lstm_bias[None], cell_state.transpose(1, 0, 2),
        context_weight.T, mlp_weight, wg, wu, wd, gg, gu, gd, meta_tokens[0],
    )
    count = lax.axis_size(TASK)
    theirs = swapped(send)
    keep = kept(info, meta_tokens[0], new_g, new_u, new_d)
    part = loss_part(info, keep, theirs, meta_targets[0], count)
    everyone = lax.all_to_all(spread(part, count), TASK, 0, 0, tiled=True)
    meta_loss = jnp.sum(everyone)
    return (
        up_g[None], up_u[None], up_d[None], new_hidden.transpose(1, 0, 2), new_cell.transpose(1, 0, 2), meta_loss
    )


def solution(mesh):
    finer = Mesh(mesh.devices.reshape(4, 4, 8, mesh.shape["shard"]), (X, Y, Z, SHARD))
    return jax.shard_map(
        local,
        mesh=finer,
        in_specs=(
            P(TASK, None, None), P(TASK, None, None), P(TASK, None, None), P(TASK, None, None),
            P(TASK, None, "shard"), P(TASK, None, "shard"), P(TASK, "shard", None), P(TASK),
            P(TASK, None, None), P(TASK, None, None), P(TASK, None), P(), P(), P(), P(),
        ),
        out_specs=(
            P(TASK, None, "shard"), P(TASK, None, "shard"), P(TASK, "shard", None),
            P(TASK, None, None), P(TASK, None, None), P(),
        ),
        check_vma=False,
    )
```
